256 devices in a mesh: band: 64 (over z, y_hi, x), ga: 4 (over y_lo, core).
Axes of the slice: x: 4, y: 4 (y_hi: 2, y_lo: 2; y = y_hi * 2 + y_lo), z: 8, core: 2. Of those that a mesh axis runs over, the one named last changes fastest.
Arguments:
- elements: bfloat16 [2, 6144, 2048], P(None, 'band', 'ga'), may hold values from -0.75 to 0.75
- screened: bfloat16 [2, 2, 2048, 2048], P(None, None, 'ga'), may hold values from -0.09375 to 0.09375
- energies: float32 [6144], replicated, may hold values from -3 to 3
- freq_points: float32 [2], replicated, may hold values from -3 to 3
- freq_weights: float32 [2], replicated, may hold values from 0.5 to 2
- band_of_slot: int32 [6144], replicated, may hold values from 0 to 6143, each once
Outputs:
- sigma: float32 [2, 6144, 6144], P(None, 'band', 'ga')
The draws below stay inside these ranges and needn't reach their ends.
Inputs may be any that keep to these rules, and one draw needn't show every extreme that they name: `band_of_slot`: each of 0 to 6143 stands once.
All inputs are finite; a program needn't handle non-finite values.
Results may differ from the reference program's by a relative error of at most 0.0042.
Values may be sent and summed in bfloat16 or wider, within the bound.
A program may use at most 128 MiB of HBM per device.

```python
import math
import jax
import jax.numpy as jnp

NG = 2048
NW = 2
NB = 6144


def block_levels(rng, extent, split, smallest, high):
    gain = 1.0
    for axis_at, blocks in split:
        heights = jax.random.uniform(jax.random.fold_in(jax.random.fold_in(rng, 6), axis_at), (blocks,), jnp.float32, smallest / len(split), high / len(split))
        gain = gain * jnp.repeat(jnp.exp(heights), extent[axis_at] // blocks).reshape((-1,) + (1,) * (len(extent) - 1 - axis_at))
    return gain


def normal_values(rng, dims, deviation, limit, shards=(), dtype=jnp.bfloat16):
    values = deviation * jax.random.normal(rng, dims, jnp.float32)
    if shards:
        values = values * block_levels(rng, dims, shards, -0.22, 0.18)
    return jnp.clip(values, -limit, limit).astype(dtype)


def setup_inputs(seed: int = 0) -> dict:
    keys = jax.random.split(jax.random.key(seed), 7)
    elements = normal_values(keys[0], (2, NB, NG), 0.125, 0.75, ((1, 64), (2, 4)))
    screened = normal_values(keys[1], (NW, 2, NG, NG), (2 * NG) ** -0.5, 0.09375, ((2, 4),))
    energies = jnp.clip(jax.random.uniform(keys[2], (NB,), jnp.float32, -3.0, 3.0), -3.0, 3.0)
    freq_points = jnp.clip(jax.random.uniform(keys[3], (NW,), jnp.float32, -3.0, 3.0), -3.0, 3.0)
    freq_weights = jnp.clip(jnp.exp(jax.random.uniform(keys[4], (NW,), jnp.float32, math.log(0.5), math.log(2.0))), 0.5, 2.0)
    band_of_slot = jax.random.permutation(keys[5], NB).astype(jnp.int32)
    return dict(elements=elements, screened=screened, energies=energies, freq_points=freq_points, freq_weights=freq_weights, band_of_slot=band_of_slot)


def reference(elements, screened, energies, freq_points, freq_weights, band_of_slot):
    slot_energy = jnp.take(energies, band_of_slot.astype(jnp.int32))
    offset = slot_energy[None, :] - freq_points[:, None]
    screen = freq_weights[:, None] / (1.0 + 4.0 * offset * offset)
    real_part = elements[0]
    imag_part = elements[1]
    total = jnp.zeros((2, NB, NB), jnp.float32)
    for freq in range(NW):
        w_real = screened[freq, 0]
        w_imag = screened[freq, 1]
        y_real = (jnp.dot(real_part, w_real.T, preferred_element_type=jnp.float32)
                  - jnp.dot(imag_part, w_imag.T, preferred_element_type=jnp.float32)).astype(jnp.bfloat16)
        y_imag = (jnp.dot(real_part, w_imag.T, preferred_element_type=jnp.float32)
                  + jnp.dot(imag_part, w_real.T, preferred_element_type=jnp.float32)).astype(jnp.bfloat16)
        pair_real = (jnp.dot(real_part, y_real.T, preferred_element_type=jnp.float32)
                     + jnp.dot(imag_part, y_imag.T, preferred_element_type=jnp.float32))
        pair_imag = (jnp.dot(real_part, y_imag.T, preferred_element_type=jnp.float32)
                     - jnp.dot(imag_part, y_real.T, preferred_element_type=jnp.float32))
        factor = 0.5 * (screen[freq][:, None] + screen[freq][None, :])
        total = total + factor[None] * jnp.stack([pair_real, pair_imag])
    return total
```

```python
import jax
import jax.numpy as jnp
from jax import lax
from jax.experimental import pallas as pl
from jax.experimental.pallas import tpu as pltpu
from jax.sharding import Mesh
from jax.sharding import PartitionSpec as P

BAND = ("z", "yh", "x")
GA = ("yl", "c")
F32 = jnp.float32
BF16 = jnp.bfloat16


def dot_t(a, b):
    return lax.dot_general(a, b, (((1,), (1,)), ((), ())), preferred_element_type=F32)


def kernel(
    elements, screened, energies, bands, points, weights, out,
    e_full, e_plane, w_buf, acc, y_buf, y_swap, s_sum, x_send, x_recv, o_buf, o_recv, s_col, s_row,
    load_sem, p_send, p_recv, a_send, a_recv, xr_send, xr_recv, z_send, z_recv,
    d_send, d_recv, o_send, o_sem,
):
    z, yh, x, yl, c = (lax.axis_index(name) for name in ("z", "yh", "x", "yl", "c"))
    own_q = yl * 2 + c
    own_b = yh * 4 + x
    slots = e_full.shape[2]

    def remote(src, dst, send, recv, **device):
        return pltpu.make_async_remote_copy(
            src_ref=src, dst_ref=dst, send_sem=send, recv_sem=recv,
            device_id=device, device_id_type=pl.DeviceIdType.MESH)

    quarter = [own_q, yl * 2 + (1 - c), (1 - yl) * 2 + c, (1 - yl) * 2 + (1 - c)]
    load_e = pltpu.make_async_copy(elements, e_full.at[own_q], load_sem.at[0])
    load_p = pltpu.make_async_copy(elements, e_plane.at[:, own_b], load_sem.at[1])
    load_e.start()
    load_p.start()
    load_w = []
    for k in range(4):
        at = pl.multiple_of(quarter[k] * 512, 512)
        load_w.append(pltpu.make_async_copy(screened.at[:, :, :, pl.ds(at, 512)], w_buf.at[k], load_sem.at[2 + k]))
        load_w[k].start()

    barrier = pltpu.get_barrier_semaphore()

    def greet(**device):
        pl.semaphore_signal(barrier, inc=1, device_id=device, device_id_type=pl.DeviceIdType.MESH)

    def plane(dyh, dx, dyl):
        return dict(yh=lax.rem(yh + dyh, 2), x=lax.rem(x + dx, 4), yl=lax.rem(yl + dyl, 2))

    greet(c=1 - c)
    z_up, z_down = lax.rem(z + 1, 8), lax.rem(z + 7, 8)
    greet(z=z_up)
    greet(z=z_down)
    for dyh in range(2):
        for dx in range(4):
            for dyl in range(2):
                if dyh or dx or dyl:
                    greet(**plane(dyh, dx, dyl))
    pl.semaphore_wait(barrier, 18)
    load_e.wait()

    to_y = remote(e_full.at[own_q], e_full.at[own_q], p_send.at[0], p_recv.at[0], yl=1 - yl)
    to_c = remote(e_full.at[own_q], e_full.at[own_q], p_send.at[1], p_recv.at[1], c=1 - c)
    to_y.start()
    to_c.start()
    load_p.wait()

    x_up, x_down = lax.rem(x + 1, 4), lax.rem(x + 3, 4)

    def block_at(k, at_x):
        return (yh if k == 0 else 1 - yh) * 4 + at_x

    def x_copy(k, way, hop):
        ahead, behind = (x_up, x_down) if way == 0 else (x_down, x_up)
        if hop == 1:
            ref = e_plane.at[:, block_at(k, x)]
        else:
            ref = e_plane.at[way, block_at(k, behind)]
        return remote(ref, ref, xr_send.at[k, way, hop - 1], xr_recv.at[k, way, hop - 1], x=ahead)

    for way in range(2):
        x_copy(0, way, 1).start()

    def accumulate(k, first):
        lhs = e_full[quarter[k]].reshape(2 * slots, 512)

        def one(i, carry):
            term = dot_t(lhs, w_buf[k, i // 2, i % 2])
            acc[i] = term if first else acc[i] + term
            return carry

        lax.fori_loop(0, 4, one, 0)

    load_w[0].wait()
    accumulate(0, True)

    def look_up(i, carry):
        at = jnp.where(i < 8, z * 8 + i, (i - 8) * 8 + own_b)
        band = jnp.broadcast_to(bands[pl.ds(at, 1), :], (128, slots)).T
        lane = lax.broadcasted_iota(jnp.int32, (slots, 128), 1)

        def part(j, total):
            for u in range(4):
                row = j * 4 + u
                e = jnp.broadcast_to(energies[pl.ds(row, 1), :], (slots, 128))
                total = total + jnp.where(band == lane + row * 128, e, 0.0)
            return total

        total = lax.fori_loop(0, 12, part, jnp.zeros((slots, 128), F32))
        energy = jnp.broadcast_to(jnp.sum(total, axis=1, keepdims=True), (slots, 128))
        for w in range(2):
            offset = energy - points[w]
            s_col[w, i] = weights[w] / (1.0 + 4.0 * offset * offset)
        return carry

    lax.fori_loop(0, 16, look_up, 0)

    def turn(i, carry):
        w, g = i // 4, i % 4
        one, two = s_col[w, 8 + 2 * g], s_col[w, 9 + 2 * g]
        s_row[w, g] = jnp.concatenate([one, one, two, two], axis=0).T[0:8]
        return carry

    lax.fori_loop(0, 8, turn, 0)

    to_c.wait_recv()
    load_w[1].wait()
    accumulate(1, False)

    to_y.wait_recv()
    other = e_full.at[quarter[2]]
    pass_c = remote(other, other, p_send.at[2], p_recv.at[2], c=1 - c)
    pass_c.start()
    to_a = remote(other, e_plane.at[:, own_b], a_send, a_recv, yh=1 - yh, yl=1 - yl)
    to_a.start()
    load_w[2].wait()
    accumulate(2, False)
    load_w[3].wait()
    pass_c.wait_recv()

    def z_copy(way, hop, w):
        ahead = z_up if way == 0 else z_down
        owner = lax.rem(z + 8 - (hop - 1), 8) if way == 0 else lax.rem(z + hop - 1, 8)
        ref = y_buf.at[w, owner]
        return remote(ref, ref, z_send.at[way, hop - 1, w], z_recv.at[way, hop - 1, w], z=ahead)

    lhs = e_full[quarter[3]].reshape(2 * slots, 512)
    for w in range(2):
        real = acc[2 * w] + dot_t(lhs, w_buf[3, w, 0])
        imag = acc[2 * w + 1] + dot_t(lhs, w_buf[3, w, 1])
        y_buf[w, z, 0] = (real[:slots] - imag[slots:]).astype(BF16)
        y_buf[w, z, 1] = (imag[:slots] + real[slots:]).astype(BF16)
        for way in range(2):
            z_copy(way, 1, w).start()

    def z_pass(hop, w):
        for way in range(2):
            if hop < 4 or way == w:
                z_copy(way, hop, w).wait_recv()
                if hop < 3 or (hop == 3 and way == w):
                    z_copy(way, hop + 1, w).start()

    def x_pass(k):
        for way in range(2):
            x_copy(k, way, 1).wait_recv()
            x_copy(k, way, 2).start()

    x_pass(0)
    remote(other, e_plane.at[:, own_b], a_send, a_recv, yh=1 - yh, yl=1 - yl).wait_recv()
    for way in range(2):
        x_copy(1, way, 1).start()
    z_pass(1, 0)
    x_pass(1)
    z_pass(1, 1)
    for k in range(2):
        for way in range(2):
            x_copy(k, way, 2).wait_recv()

    pair = z // 2
    even = lax.rem(z, 2) == 0

    def products(g):
        def swap(i, carry):
            w, j = i // 2, i % 2
            y_swap[w, j, 0] = y_buf[w, 2 * g + j, 1]
            y_swap[w, j, 1] = -y_buf[w, 2 * g + j, 0]
            return carry

        lax.fori_loop(0, 4, swap, 0)

        def rows(i, carry):
            real = e_plane[0, pl.ds(i * 4, 4)].reshape(4 * slots, 512)
            imag = e_plane[1, pl.ds(i * 4, 4)].reshape(4 * slots, 512)
            total = None
            for w in range(2):
                straight = y_buf[w, pl.ds(2 * g, 2)].reshape(4 * slots, 512)
                swapped = y_swap[w].reshape(4 * slots, 512)
                both = dot_t(real, straight) + dot_t(imag, swapped)
                s = s_col[w, pl.ds(i * 4, 4)].reshape(4 * slots, 128)
                factor = 0.5 * (jnp.concatenate([s, s, s], axis=1) + s_row[w, g][0:1])
                total = both * factor if total is None else total + both * factor
            s_sum[pl.ds(i * 4, 4)] = total.reshape(4, slots, 4 * slots)
            return carry

        lax.fori_loop(0, 2, rows, 0)

    def out_copy(slot, dyh, dx, to_yl):
        to_yh, to_x = lax.rem(yh + dyh, 2), lax.rem(x + dx, 4)
        index = yl * 8 + own_b
        return remote(o_buf.at[slot, to_yh * 4 + to_x], o_recv.at[index], o_send.at[slot, dyh * 4 + dx], o_sem.at[index],
                      yh=to_yh, x=to_x, yl=to_yl)

    places = [lax.rem(pair, 4),
              jnp.where(even, lax.rem(pair + 3, 4), lax.rem(pair + 1, 4)),
              jnp.where(even, lax.rem(pair + 1, 4), lax.rem(pair + 3, 4)),
              lax.rem(pair + 2, 4)]
    slot_of = [0, 0, 1, 1]

    def finish(t):
        g, slot = places[t], slot_of[t]
        products(g)
        mine = lax.rem(g, 2) == c
        across = remote(x_send.at[slot], x_recv.at[slot], d_send.at[slot], d_recv.at[slot], c=1 - c)

        @pl.when(jnp.logical_not(mine))
        def _():
            x_send[slot] = s_sum[...].astype(BF16)
            across.start()

        @pl.when(mine)
        def _():
            across.wait_recv()
            o_buf[slot] = (s_sum[...] + x_recv[slot].astype(F32)).astype(BF16)
            to_yl = g // 2
            for dyh in range(2):
                for dx in range(4):
                    if dyh or dx:
                        out_copy(slot, dyh, dx, to_yl).start()

            @pl.when(to_yl == yl)
            def _():
                o_recv[yl * 8 + own_b] = o_buf[slot, own_b]

            @pl.when(to_yl != yl)
            def _():
                out_copy(slot, 0, 0, to_yl).start()

    finish(0)
    z_pass(2, 0)
    z_pass(2, 1)
    finish(1)
    z_pass(3, 0)
    z_pass(3, 1)
    finish(2)
    z_pass(4, 0)
    z_pass(4, 1)
    finish(3)

    for dyh in range(2):
        for dx in range(4):
            for dyl in range(2):
                if dyh or dx or dyl:
                    index = lax.rem(yl + dyl, 2) * 8 + lax.rem(yh + dyh, 2) * 4 + lax.rem(x + dx, 4)
                    remote(o_buf.at[0, 0], o_recv.at[index], o_send.at[0, 0], o_sem.at[index], c=1 - c).wait_recv()

    for b in range(8):
        block = o_recv[b].astype(F32) + o_recv[8 + b].astype(F32)
        for j in range(2):
            for part in range(2):
                at = (j * 2 + part) * slots
                to = j * 8 * slots + b * slots
                out[part, :, to:to + slots] = block[:, at:at + slots]

    to_y.wait_send()
    to_c.wait_send()
    pass_c.wait_send()
    to_a.wait_send()
    for k in range(2):
        for way in range(2):
            for hop in (1, 2):
                x_copy(k, way, hop).wait_send()
    for way in range(2):
        for hop in range(1, 5):
            for w in range(2):
                if hop < 4 or way == w:
                    z_copy(way, hop, w).wait_send()
    for t in range(4):
        g, slot = places[t], slot_of[t]
        mine = lax.rem(g, 2) == c

        @pl.when(jnp.logical_not(mine))
        def _():
            remote(x_send.at[slot], x_recv.at[slot], d_send.at[slot], d_recv.at[slot], c=1 - c).wait_send()

        @pl.when(mine)
        def _():
            for dyh in range(2):
                for dx in range(4):
                    if dyh or dx:
                        out_copy(slot, dyh, dx, g // 2).wait_send()

            @pl.when(g // 2 != yl)
            def _():
                out_copy(slot, 0, 0, g // 2).wait_send()


def on_device(elements, screened, energies, freq_points, freq_weights, band_of_slot):
    slots = elements.shape[1]
    vmem = pl.BlockSpec(memory_space=pltpu.VMEM)
    smem = pl.BlockSpec(memory_space=pltpu.SMEM)
    anywhere = pl.BlockSpec(memory_space=pl.ANY)
    dma = pltpu.SemaphoreType.DMA
    return pl.pallas_call(
        kernel,
        out_shape=jax.ShapeDtypeStruct((2, slots, 16 * slots), F32),
        in_specs=[anywhere, anywhere, vmem, vmem, smem, smem],
        out_specs=vmem,
        scratch_shapes=[
            pltpu.VMEM((4, 2, slots, 512), BF16),
            pltpu.VMEM((2, 8, slots, 512), BF16),
            pltpu.VMEM((4, 2, 2, 512, 512), BF16),
            pltpu.VMEM((4, 2 * slots, 512), F32),
            pltpu.VMEM((2, 8, 2, slots, 512), BF16),
            pltpu.VMEM((2, 2, 2, slots, 512), BF16),
            pltpu.VMEM((8, slots, 4 * slots), F32),
            pltpu.VMEM((2, 8, slots, 4 * slots), BF16),
            pltpu.VMEM((2, 8, slots, 4 * slots), BF16),
            pltpu.VMEM((2, 8, slots, 4 * slots), BF16),
            pltpu.VMEM((16, slots, 4 * slots), BF16),
            pltpu.VMEM((2, 16, slots, 128), F32),
            pltpu.VMEM((2, 4, 8, 4 * slots), F32),
            dma((6,)), dma((3,)), dma((3,)), dma, dma,
            dma((2, 2, 2)), dma((2, 2, 2)), dma((2, 4, 2)), dma((2, 4, 2)),
            dma((2,)), dma((2,)), dma((2, 8)), dma((16,)),
        ],
        compiler_params=pltpu.CompilerParams(
            collective_id=0, has_side_effects=True, vmem_limit_bytes=60 * 1024 * 1024),
        name="self_energy",
    )(elements, screened, energies.reshape(48, 128), band_of_slot.reshape(64, slots), freq_points, freq_weights)


def solution(mesh):
    torus = Mesh(mesh.devices.reshape(8, 2, 4, 2, 2), ("z", "yh", "x", "yl", "c"))
    return jax.shard_map(
        on_device,
        mesh=torus,
        in_specs=(P(None, BAND, GA), P(None, None, GA, None), P(), P(), P(), P()),
        out_specs=P(None, BAND, GA),
        check_vma=False,
    )
```

```python
import jax
import jax.numpy as jnp
from jax import lax
from jax.experimental import pallas as pl
from jax.experimental.pallas import tpu as pltpu
from jax.sharding import Mesh
from jax.sharding import PartitionSpec as P

BAND = ("z", "yh", "x")
GA = ("yl", "c")
F32 = jnp.float32
BF16 = jnp.bfloat16
scope = jax.named_scope


def dot_t(a, b):
    return lax.dot_general(a, b, (((1,), (1,)), ((), ())), preferred_element_type=F32)


def kernel(
    elements, screened, energies, bands, points, weights, out,
    e_full, e_plane, w_buf, acc, y_buf, y_swap, s_sum, x_send, x_recv, o_buf, o_recv, s_col, s_row,
    energy_buf, band_buf, band_table, point_buf, weight_buf,
    load_sem, p_send, p_recv, a_send, a_recv, xr_send, xr_recv, z_send, z_recv,
    d_send, d_recv, o_send, o_sem,
):
    z, yh, x, yl, c = (lax.axis_index(name) for name in ("z", "yh", "x", "yl", "c"))
    own_q = yl * 2 + c
    own_b = yh * 4 + x
    slots = e_full.shape[2]

    def remote(src, dst, send, recv, **device):
        return pltpu.make_async_remote_copy(
            src_ref=src, dst_ref=dst, send_sem=send, recv_sem=recv,
            device_id=device, device_id_type=pl.DeviceIdType.MESH)

    quarter = [own_q, yl * 2 + (1 - c), (1 - yl) * 2 + c, (1 - yl) * 2 + (1 - c)]
    load_e = pltpu.make_async_copy(elements, e_full.at[own_q], load_sem.at[0])
    load_p = pltpu.make_async_copy(elements, e_plane.at[:, own_b], load_sem.at[1])
    load_e.start()
    load_p.start()
    load_s = [pltpu.make_async_copy(src, dst, load_sem.at[6 + i]) for i, (src, dst) in enumerate(
        ((energies, energy_buf), (bands, band_buf), (points, point_buf), (weights, weight_buf)))]
    load_w = []
    for k in range(4):
        at = pl.multiple_of(quarter[k] * 512, 512)
        load_w.append(pltpu.make_async_copy(screened.at[:, :, :, pl.ds(at, 512)], w_buf.at[k], load_sem.at[2 + k]))
        load_w[k].start()
    for load in load_s:
        load.start()

    barrier = pltpu.get_barrier_semaphore()

    def greet(**device):
        pl.semaphore_signal(barrier, inc=1, device_id=device, device_id_type=pl.DeviceIdType.MESH)

    def plane(dyh, dx, dyl):
        return dict(yh=lax.rem(yh + dyh, 2), x=lax.rem(x + dx, 4), yl=lax.rem(yl + dyl, 2))

    greet(c=1 - c)
    z_up, z_down = lax.rem(z + 1, 8), lax.rem(z + 7, 8)
    greet(z=z_up)
    greet(z=z_down)
    for dyh in range(2):
        for dx in range(4):
            for dyl in range(2):
                if dyh or dx or dyl:
                    greet(**plane(dyh, dx, dyl))
    with scope("enter"):
        pl.semaphore_wait(barrier, 18)
        load_e.wait()

    to_y = remote(e_full.at[own_q], e_full.at[own_q], p_send.at[0], p_recv.at[0], yl=1 - yl)
    to_c = remote(e_full.at[own_q], e_full.at[own_q], p_send.at[1], p_recv.at[1], c=1 - c)
    to_y.start()
    to_c.start()
    load_p.wait()

    x_up, x_down = lax.rem(x + 1, 4), lax.rem(x + 3, 4)

    def block_at(k, at_x):
        return (yh if k == 0 else 1 - yh) * 4 + at_x

    def x_copy(k, way, hop):
        ahead, behind = (x_up, x_down) if way == 0 else (x_down, x_up)
        if hop == 1:
            ref = e_plane.at[:, block_at(k, x)]
        else:
            ref = e_plane.at[way, block_at(k, behind)]
        return remote(ref, ref, xr_send.at[k, way, hop - 1], xr_recv.at[k, way, hop - 1], x=ahead)

    for way in range(2):
        x_copy(0, way, 1).start()

    def accumulate(k, first):
        lhs = e_full[quarter[k]].reshape(2 * slots, 512)

        for i in range(4):
            term = dot_t(lhs, w_buf[k, i // 2, i % 2])
            acc[i] = term if first else acc[i] + term

    with scope("quarter0"):
        load_w[0].wait()
        accumulate(0, True)

    with scope("quarter1"):
        to_c.wait_recv()
        load_w[1].wait()
        accumulate(1, False)

    with scope("wait_y"):
        to_y.wait_recv()
    other = e_full.at[quarter[2]]
    pass_c = remote(other, other, p_send.at[2], p_recv.at[2], c=1 - c)
    pass_c.start()
    to_a = remote(other, e_plane.at[:, own_b], a_send, a_recv, yh=1 - yh, yl=1 - yl)
    to_a.start()
    with scope("quarter2"):
        load_w[2].wait()
        accumulate(2, False)
        load_w[3].wait()
    with scope("wait_c"):
        pass_c.wait_recv()

    def z_copy(way, hop, w):
        ahead = z_up if way == 0 else z_down
        owner = lax.rem(z + 8 - (hop - 1), 8) if way == 0 else lax.rem(z + hop - 1, 8)
        ref = y_buf.at[w, owner]
        return remote(ref, ref, z_send.at[way, hop - 1, w], z_recv.at[way, hop - 1, w], z=ahead)

    with scope("applied"):
        lhs = e_full[quarter[3]].reshape(2 * slots, 512)
        for w in range(2):
            real = acc[2 * w] + dot_t(lhs, w_buf[3, w, 0])
            imag = acc[2 * w + 1] + dot_t(lhs, w_buf[3, w, 1])
            y_buf[w, z, 0] = (real[:slots] - imag[slots:]).astype(BF16)
            y_buf[w, z, 1] = (imag[:slots] + real[slots:]).astype(BF16)
            for way in range(2):
                z_copy(way, 1, w).start()

    def z_pass(hop, w):
        for way in range(2):
            if hop < 4 or way == w:
                z_copy(way, hop, w).wait_recv()
                if hop < 3 or (hop == 3 and way == w):
                    z_copy(way, hop + 1, w).start()

    def x_pass(k):
        for way in range(2):
            x_copy(k, way, 1).wait_recv()
            x_copy(k, way, 2).start()

    def spread_bands():
        rows = [band_buf[pl.ds(k, 16, stride=3), :] for k in range(3)]
        band_table[0] = rows[0]
        band_table[1] = jnp.concatenate([rows[0][:, 96:], rows[1][:, :96]], axis=1)
        band_table[2] = jnp.concatenate([rows[1][:, 64:], rows[2][:, :64]], axis=1)
        band_table[3] = jnp.concatenate([rows[2][:, 32:], rows[2][:, :32]], axis=1)

    def look_up(i, carry):
        at = jnp.where(i < 8, z * 8 + i, (i - 8) * 8 + own_b)
        band = band_table[lax.rem(at, 4), pl.ds(at // 4, 1), :]
        band = jnp.broadcast_to(band, (128, 128)).T[:slots]
        lane = lax.broadcasted_iota(jnp.int32, (slots, 128), 1)

        def part(j, total):
            for u in range(8):
                row = j * 8 + u
                e = jnp.broadcast_to(energy_buf[pl.ds(row, 1), :], (slots, 128))
                total = total + jnp.where(band == lane + row * 128, e, 0.0)
            return total

        total = lax.fori_loop(0, 6, part, jnp.zeros((slots, 128), F32))
        energy = jnp.broadcast_to(jnp.sum(total, axis=1, keepdims=True), (slots, 128))
        for w in range(2):
            offset = energy - point_buf[w]
            s_col[w, i] = weight_buf[w] / (1.0 + 4.0 * offset * offset)
        return carry

    def turn(i, carry):
        w, g = i // 8, lax.rem(i, 8)
        one = s_col[w, 8 + g]
        s_row[w, g] = jnp.concatenate([one, one], axis=0).T[0:8]
        return carry

    with scope("x_pass0"):
        x_pass(0)
    with scope("look_up0"):
        for load in load_s:
            load.wait()
        spread_bands()
        lax.fori_loop(0, 8, look_up, 0)
    with scope("wait_a"):
        remote(other, e_plane.at[:, own_b], a_send, a_recv, yh=1 - yh, yl=1 - yl).wait_recv()
    for way in range(2):
        x_copy(1, way, 1).start()
    with scope("z10"):
        z_pass(1, 0)
    with scope("look_up1"):
        lax.fori_loop(8, 16, look_up, 0)
        lax.fori_loop(0, 16, turn, 0)
    with scope("x_pass1"):
        x_pass(1)
    with scope("z11"):
        z_pass(1, 1)
    with scope("wait_x"):
        for k in range(2):
            for way in range(2):
                x_copy(k, way, 2).wait_recv()

    half = slots // 2
    deltas = (0, 7, 1, 6, 2, 5, 3, 4)

    def block_z(t):
        return lax.rem(z + deltas[t], 8)

    def mine(t):
        return lax.rem(block_z(t) // 2, 2) == c

    def across(t):
        return remote(x_send.at[t], x_recv.at[t], d_send.at[t], d_recv.at[t], c=1 - c)

    @scope("products")
    def products(t):
        zz = block_z(t)
        for w in range(2):
            y_swap[w, 0] = y_buf[w, zz, 1]
            y_swap[w, 1] = -y_buf[w, zz, 0]
        for i in range(2):
            real = e_plane[0, i * 4:i * 4 + 4].reshape(4 * slots, 512)
            imag = e_plane[1, i * 4:i * 4 + 4].reshape(4 * slots, 512)
            total = None
            for w in range(2):
                both = dot_t(real, y_buf[w, zz].reshape(2 * slots, 512)) + dot_t(imag, y_swap[w].reshape(2 * slots, 512))
                s = s_col[w, i * 4:i * 4 + 4].reshape(4 * slots, 128)
                factor = 0.5 * (jnp.concatenate([s, s[:, :2 * slots - 128]], axis=1) + s_row[w, zz][0:1])
                total = both * factor if total is None else total + both * factor
            total = total.reshape(4, slots, 2 * slots)
            s_sum[t % 2, i * 4:i * 4 + 4] = jnp.concatenate([total[:, :half], total[:, half:]], axis=2)

        @pl.when(jnp.logical_not(mine(t)))
        def _():
            x_send[t] = s_sum[t % 2].astype(BF16)
            across(t).start()

    def out_copy(t, dyh, dx):
        zz = block_z(t)
        to_yh, to_x = lax.rem(yh + dyh, 2), lax.rem(x + dx, 4)
        index, column = yl * 8 + own_b, lax.rem(zz, 2)
        return remote(o_buf.at[t, to_yh * 4 + to_x], o_recv.at[column, index], o_send.at[t, dyh * 4 + dx],
                      o_sem.at[column, index], yh=to_yh, x=to_x, yl=zz // 4)

    @scope("complete")
    def complete(t):
        @pl.when(mine(t))
        def _():
            across(t).wait_recv()
            o_buf[t] = (s_sum[t % 2] + x_recv[t].astype(F32)).astype(BF16)
            for dx in (2, 1, 3, 0):
                for dyh in (1, 0):
                    if dyh or dx:
                        out_copy(t, dyh, dx).start()

            @pl.when(block_z(t) // 4 == yl)
            def _():
                o_recv[lax.rem(block_z(t), 2), yl * 8 + own_b] = o_buf[t, own_b]

            @pl.when(block_z(t) // 4 != yl)
            def _():
                out_copy(t, 0, 0).start()

    products(0)
    z_pass(2, 0)
    products(1)
    complete(0)
    with scope("z21"):
        z_pass(2, 1)
    products(2)
    complete(1)
    products(3)
    complete(2)
    with scope("z30"):
        z_pass(3, 0)
    products(4)
    complete(3)
    with scope("z31"):
        z_pass(3, 1)
    products(5)
    complete(4)
    products(6)
    complete(5)
    with scope("z40"):
        z_pass(4, 0)
    complete(6)
    with scope("z41"):
        z_pass(4, 1)
    products(7)
    complete(7)

    with scope("wait_out"):
        for column in range(2):
            for dyh in range(2):
                for dx in range(4):
                    for dyl in range(2):
                        if dyh or dx or dyl:
                            index = lax.rem(yl + dyl, 2) * 8 + lax.rem(yh + dyh, 2) * 4 + lax.rem(x + dx, 4)
                            remote(o_buf.at[0, 0], o_recv.at[column, index], o_send.at[0, 0],
                                   o_sem.at[column, index], c=1 - c).wait_recv()

    with scope("lay_out"):
        for column in range(2):
            for b in range(8):
                block = o_recv[column, b].astype(F32) + o_recv[column, 8 + b].astype(F32)
                to = (column * 8 + b) * slots
                for part in range(2):
                    for low in range(2):
                        at = (low * 2 + part) * slots
                        out[part, low * half:low * half + half, to:to + slots] = block[:, at:at + slots]

    to_y.wait_send()
    to_c.wait_send()
    pass_c.wait_send()
    to_a.wait_send()
    for k in range(2):
        for way in range(2):
            for hop in (1, 2):
                x_copy(k, way, hop).wait_send()
    for way in range(2):
        for hop in range(1, 5):
            for w in range(2):
                if hop < 4 or way == w:
                    z_copy(way, hop, w).wait_send()
    for t in range(8):
        @pl.when(jnp.logical_not(mine(t)))
        def _():
            across(t).wait_send()

        @pl.when(mine(t))
        def _():
            for dyh in range(2):
                for dx in range(4):
                    if dyh or dx:
                        out_copy(t, dyh, dx).wait_send()

            @pl.when(block_z(t) // 4 != yl)
            def _():
                out_copy(t, 0, 0).wait_send()


def on_device(elements, screened, energies, freq_points, freq_weights, band_of_slot):
    slots = elements.shape[1]
    half = slots // 2
    vmem = pl.BlockSpec(memory_space=pltpu.VMEM)
    anywhere = pl.BlockSpec(memory_space=pl.ANY)
    dma = pltpu.SemaphoreType.DMA
    return pl.pallas_call(
        kernel,
        out_shape=jax.ShapeDtypeStruct((2, slots, 16 * slots), F32),
        in_specs=[anywhere] * 6,
        out_specs=vmem,
        scratch_shapes=[
            pltpu.VMEM((4, 2, slots, 512), BF16),
            pltpu.VMEM((2, 8, slots, 512), BF16),
            pltpu.VMEM((4, 2, 2, 512, 512), BF16),
            pltpu.VMEM((4, 2 * slots, 512), F32),
            pltpu.VMEM((2, 8, 2, slots, 512), BF16),
            pltpu.VMEM((2, 2, slots, 512), BF16),
            pltpu.VMEM((2, 8, half, 4 * slots), F32),
            pltpu.VMEM((8, 8, half, 4 * slots), BF16),
            pltpu.VMEM((8, 8, half, 4 * slots), BF16),
            pltpu.VMEM((8, 8, half, 4 * slots), BF16),
            pltpu.VMEM((2, 16, half, 4 * slots), BF16),
            pltpu.VMEM((2, 16, slots, 128), F32),
            pltpu.VMEM((2, 8, 8, 2 * slots), F32),
            pltpu.VMEM((48, 128), F32),
            pltpu.VMEM((48, 128), jnp.int32),
            pltpu.VMEM((4, 16, 128), jnp.int32),
            pltpu.SMEM((2,), F32), pltpu.SMEM((2,), F32),
            dma((10,)), dma((3,)), dma((3,)), dma, dma,
            dma((2, 2, 2)), dma((2, 2, 2)), dma((2, 4, 2)), dma((2, 4, 2)),
            dma((8,)), dma((8,)), dma((8, 8)), dma((2, 16)),
        ],
        compiler_params=pltpu.CompilerParams(
            collective_id=0, has_side_effects=True, vmem_limit_bytes=60 * 1024 * 1024),
        name="self_energy",
    )(elements, screened, energies.reshape(48, 128), band_of_slot.reshape(48, 128), freq_points, freq_weights)


def solution(mesh):
    torus = Mesh(mesh.devices.reshape(8, 2, 4, 2, 2), ("z", "yh", "x", "yl", "c"))
    return jax.shard_map(
        on_device,
        mesh=torus,
        in_specs=(P(None, BAND, GA), P(None, None, GA, None), P(), P(), P(), P()),
        out_specs=P(None, BAND, GA),
        check_vma=False,
    )
```

```python
import jax
import jax.numpy as jnp
from jax import lax
from jax.experimental import pallas as pl
from jax.experimental.pallas import tpu as pltpu
from jax.sharding import Mesh
from jax.sharding import PartitionSpec as P

BAND = ("z", "yh", "x")
GA = ("yl", "c")
F32 = jnp.float32
BF16 = jnp.bfloat16
scope = jax.named_scope


def dot_t(a, b):
    return lax.dot_general(a, b, (((1,), (1,)), ((), ())), preferred_element_type=F32)


def kernel(
    elements, screened, energies, bands, points, weights, o_recv,
    e_full, e_plane, w_buf, acc, y_buf, y_swap, s_sum, x_send, x_recv, o_buf, s_col, s_row,
    energy_buf, band_buf, band_table, point_buf, weight_buf,
    load_sem, keep_sem, p_send, p_recv, a_send, a_recv, xr_send, xr_recv, z_send, z_recv,
    d_send, d_recv, o_send, o_sem,
):
    z, yh, x, yl, c = (lax.axis_index(name) for name in ("z", "yh", "x", "yl", "c"))
    own_q = yl * 2 + c
    own_b = yh * 4 + x
    slots = e_full.shape[2]

    def remote(src, dst, send, recv, **device):
        return pltpu.make_async_remote_copy(
            src_ref=src, dst_ref=dst, send_sem=send, recv_sem=recv,
            device_id=device, device_id_type=pl.DeviceIdType.MESH)

    quarter = [own_q, yl * 2 + (1 - c), (1 - yl) * 2 + c, (1 - yl) * 2 + (1 - c)]
    load_e = pltpu.make_async_copy(elements, e_full.at[own_q], load_sem.at[0])
    load_p = pltpu.make_async_copy(elements, e_plane.at[:, own_b], load_sem.at[1])
    load_e.start()
    load_p.start()
    load_s = [pltpu.make_async_copy(src, dst, load_sem.at[6 + i]) for i, (src, dst) in enumerate(
        ((energies, energy_buf), (bands, band_buf), (points, point_buf), (weights, weight_buf)))]
    load_w = []
    for k in range(4):
        at = pl.multiple_of(quarter[k] * 512, 512)
        load_w.append(pltpu.make_async_copy(screened.at[:, :, :, pl.ds(at, 512)], w_buf.at[k], load_sem.at[2 + k]))
        load_w[k].start()
    for load in load_s:
        load.start()

    barrier = pltpu.get_barrier_semaphore()

    def greet(**device):
        pl.semaphore_signal(barrier, inc=1, device_id=device, device_id_type=pl.DeviceIdType.MESH)

    def plane(dyh, dx, dyl):
        return dict(yh=lax.rem(yh + dyh, 2), x=lax.rem(x + dx, 4), yl=lax.rem(yl + dyl, 2))

    greet(c=1 - c)
    z_up, z_down = lax.rem(z + 1, 8), lax.rem(z + 7, 8)
    greet(z=z_up)
    greet(z=z_down)
    greet(yl=1 - yl)
    greet(yh=1 - yh, yl=1 - yl)
    greet(x=lax.rem(x + 1, 4))
    greet(x=lax.rem(x + 3, 4))
    with scope("enter"):
        pl.semaphore_wait(barrier, 7)
        load_e.wait()

    def to_y(h):
        ref = e_full.at[own_q, :, :, pl.ds(h * 256, 256)]
        return remote(ref, ref, p_send.at[2 * h], p_recv.at[2 * h], yl=1 - yl)

    to_c = remote(e_full.at[own_q], e_full.at[own_q], p_send.at[4], p_recv.at[4], c=1 - c)
    to_y(0).start()
    to_y(1).start()
    to_c.start()
    load_p.wait()

    x_up, x_down = lax.rem(x + 1, 4), lax.rem(x + 3, 4)

    def block_at(k, at_x):
        return (yh if k == 0 else 1 - yh) * 4 + at_x

    def x_copy(k, way, hop):
        ahead, behind = (x_up, x_down) if way == 0 else (x_down, x_up)
        if hop == 1:
            ref = e_plane.at[:, block_at(k, x)]
        else:
            ref = e_plane.at[way, block_at(k, behind)]
        return remote(ref, ref, xr_send.at[k, way, hop - 1], xr_recv.at[k, way, hop - 1], x=ahead)

    for way in range(2):
        x_copy(0, way, 1).start()

    def terms(k, w, part, low, size):
        lhs = e_full[quarter[k], :, :, low:low + size].reshape(2 * slots, size)
        return dot_t(lhs, w_buf[k, w, part, :, low:low + size])

    def accumulate(k, low=0, size=512):
        for i in range(4):
            term = terms(k, i // 2, i % 2, low, size)
            acc[i] = term if k == 0 else acc[i] + term

    with scope("quarter0"):
        load_w[0].wait()
        accumulate(0)

    with scope("quarter1"):
        to_c.wait_recv()
        load_w[1].wait()
        accumulate(1)

    def pass_c(h):
        ref = e_full.at[quarter[2], :, :, pl.ds(h * 256, 256)]
        return remote(ref, ref, p_send.at[2 * h + 1], p_recv.at[2 * h + 1], c=1 - c)

    other = e_full.at[quarter[2]]
    to_a = remote(other, e_plane.at[:, own_b], a_send, a_recv, yh=1 - yh, yl=1 - yl)
    load_w[2].wait()
    load_w[3].wait()
    with scope("wait_y0"):
        to_y(0).wait_recv()
    pass_c(0).start()
    with scope("quarter2"):
        accumulate(2, 0, 256)
    with scope("wait_y1"):
        to_y(1).wait_recv()
    pass_c(1).start()
    to_a.start()
    with scope("quarter3"):
        accumulate(2, 256, 256)
        pass_c(0).wait_recv()
        accumulate(3, 0, 256)
    with scope("wait_c"):
        pass_c(1).wait_recv()

    def z_copy(way, hop, w):
        ahead = z_up if way == 0 else z_down
        owner = lax.rem(z + 8 - (hop - 1), 8) if way == 0 else lax.rem(z + hop - 1, 8)
        ref = y_buf.at[w, owner]
        return remote(ref, ref, z_send.at[way, hop - 1, w], z_recv.at[way, hop - 1, w], z=ahead)

    with scope("applied"):
        for w in range(2):
            real = acc[2 * w] + terms(3, w, 0, 256, 256)
            imag = acc[2 * w + 1] + terms(3, w, 1, 256, 256)
            y_buf[w, z, 0] = (real[:slots] - imag[slots:]).astype(BF16)
            y_buf[w, z, 1] = (imag[:slots] + real[slots:]).astype(BF16)
            if w == 0:
                z_copy(0, 1, 0).start()
        z_copy(1, 1, 1).start()
        z_copy(0, 1, 1).start()
        z_copy(1, 1, 0).start()

    def z_pass(hop, turn):
        for way in range(2):
            w = turn if way == 0 else 1 - turn
            z_copy(way, hop, w).wait_recv()
            if hop < 3 or (hop == 3 and turn == 0):
                z_copy(way, hop + 1, w).start()

    def x_pass(k):
        for way in range(2):
            x_copy(k, way, 1).wait_recv()
            x_copy(k, way, 2).start()

    def spread_bands():
        rows = [band_buf[pl.ds(k, 16, stride=3), :] for k in range(3)]
        band_table[0] = rows[0]
        band_table[1] = jnp.concatenate([rows[0][:, 96:], rows[1][:, :96]], axis=1)
        band_table[2] = jnp.concatenate([rows[1][:, 64:], rows[2][:, :64]], axis=1)
        band_table[3] = jnp.concatenate([rows[2][:, 32:], rows[2][:, :32]], axis=1)

    def look_up(i, carry):
        at = jnp.where(i < 8, z * 8 + i, (i - 8) * 8 + own_b)
        band = band_table[lax.rem(at, 4), pl.ds(at // 4, 1), :]
        band = jnp.broadcast_to(band, (128, 128)).T[:slots]
        lane = lax.broadcasted_iota(jnp.int32, (slots, 128), 1)

        def part(j, total):
            for u in range(8):
                row = j * 8 + u
                e = jnp.broadcast_to(energy_buf[pl.ds(row, 1), :], (slots, 128))
                total = total + jnp.where(band == lane + row * 128, e, 0.0)
            return total

        total = lax.fori_loop(0, 6, part, jnp.zeros((slots, 128), F32))
        energy = jnp.broadcast_to(jnp.sum(total, axis=1, keepdims=True), (slots, 128))
        for w in range(2):
            offset = energy - point_buf[w]
            s_col[w, i] = weight_buf[w] / (1.0 + 4.0 * offset * offset)
        return carry

    def turn(i, carry):
        w, g = i // 8, lax.rem(i, 8)
        one = s_col[w, 8 + g]
        s_row[w, g] = jnp.concatenate([one, one], axis=0).T[0:8]
        return carry

    with scope("x_pass0"):
        x_pass(0)
    with scope("look_up0"):
        for load in load_s:
            load.wait()
        spread_bands()
        lax.fori_loop(0, 8, look_up, 0)
    with scope("wait_a"):
        remote(other, e_plane.at[:, own_b], a_send, a_recv, yh=1 - yh, yl=1 - yl).wait_recv()
    for way in range(2):
        x_copy(1, way, 1).start()
    with scope("z10"):
        z_pass(1, 0)
    with scope("look_up1"):
        lax.fori_loop(8, 16, look_up, 0)
    with scope("x_pass1"):
        x_pass(1)
    with scope("z11"):
        z_pass(1, 1)
    with scope("turn"):
        lax.fori_loop(0, 16, turn, 0)
    with scope("z20"):
        z_pass(2, 0)
    with scope("wait_x"):
        for k in range(2):
            for way in range(2):
                x_copy(k, way, 2).wait_recv()

    half = slots // 2
    deltas = (0, 7, 1, 6, 2, 5, 3, 4)

    def block_z(t):
        return lax.rem(z + deltas[t], 8)

    def mine(t):
        return lax.rem(block_z(t) // 2, 2) == c

    def across(t):
        return remote(x_send.at[t], x_recv.at[t], d_send.at[t], d_recv.at[t], c=1 - c)

    @scope("products")
    def products(t):
        zz = block_z(t)
        for w in range(2):
            y_swap[w, 0] = y_buf[w, zz, 1]
            y_swap[w, 1] = -y_buf[w, zz, 0]
        for i in range(2):
            real = e_plane[0, i * 4:i * 4 + 4].reshape(4 * slots, 512)
            imag = e_plane[1, i * 4:i * 4 + 4].reshape(4 * slots, 512)
            total = None
            for w in range(2):
                both = dot_t(real, y_buf[w, zz].reshape(2 * slots, 512)) + dot_t(imag, y_swap[w].reshape(2 * slots, 512))
                s = s_col[w, i * 4:i * 4 + 4].reshape(4 * slots, 128)
                factor = 0.5 * (jnp.concatenate([s, s[:, :2 * slots - 128]], axis=1) + s_row[w, zz][0:1])
                total = both * factor if total is None else total + both * factor
            total = total.reshape(4, slots, 2 * slots)
            s_sum[t % 2, i * 4:i * 4 + 4] = jnp.concatenate([total[:, :half], total[:, half:]], axis=2)

        @pl.when(jnp.logical_not(mine(t)))
        def _():
            x_send[t] = s_sum[t % 2].astype(BF16)
            across(t).start()

    def out_copy(t, dyh, dx):
        zz = block_z(t)
        to_yh, to_x = lax.rem(yh + dyh, 2), lax.rem(x + dx, 4)
        index, column = yl * 8 + own_b, lax.rem(zz, 2)
        return remote(o_buf.at[t, to_yh * 4 + to_x], o_recv.at[column, index], o_send.at[t, dyh * 4 + dx],
                      o_sem.at[column, index], yh=to_yh, x=to_x, yl=zz // 4)

    def keep(t):
        return pltpu.make_async_copy(o_buf.at[t, own_b], o_recv.at[lax.rem(block_z(t), 2), yl * 8 + own_b], keep_sem.at[t])

    @scope("complete")
    def complete(t):
        @pl.when(mine(t))
        def _():
            across(t).wait_recv()
            o_buf[t] = (s_sum[t % 2] + x_recv[t].astype(F32)).astype(BF16)
            for dx in (2, 1, 3, 0):
                for dyh in (1, 0):
                    if dyh or dx:
                        out_copy(t, dyh, dx).start()

            @pl.when(block_z(t) // 4 == yl)
            def _():
                keep(t).start()

            @pl.when(block_z(t) // 4 != yl)
            def _():
                out_copy(t, 0, 0).start()

    products(0)
    products(1)
    complete(0)
    with scope("z21"):
        z_pass(2, 1)
    products(2)
    complete(1)
    with scope("z30"):
        z_pass(3, 0)
    products(3)
    complete(2)
    products(4)
    complete(3)
    with scope("z31"):
        z_pass(3, 1)
    products(5)
    complete(4)
    products(6)
    complete(5)
    complete(6)
    with scope("z40"):
        z_pass(4, 0)
    products(7)
    complete(7)

    with scope("wait_out"):
        for column in range(2):
            for dyh in range(2):
                for dx in range(4):
                    for dyl in range(2):
                        if dyh or dx or dyl:
                            index = lax.rem(yl + dyl, 2) * 8 + lax.rem(yh + dyh, 2) * 4 + lax.rem(x + dx, 4)
                            remote(o_buf.at[0, 0], o_recv.at[column, index], o_send.at[0, 0],
                                   o_sem.at[column, index], c=1 - c).wait_recv()

    with scope("drain"):
        to_c.wait_send()
        for h in range(2):
            to_y(h).wait_send()
            pass_c(h).wait_send()
        to_a.wait_send()
        for k in range(2):
            for way in range(2):
                for hop in (1, 2):
                    x_copy(k, way, hop).wait_send()
        for way in range(2):
            for hop in range(1, 5):
                for w in range(2):
                    if hop < 4 or way == w:
                        z_copy(way, hop, w).wait_send()
        for t in range(8):
            @pl.when(jnp.logical_not(mine(t)))
            def _():
                across(t).wait_send()

            @pl.when(mine(t))
            def _():
                for dyh in range(2):
                    for dx in range(4):
                        if dyh or dx:
                            out_copy(t, dyh, dx).wait_send()

                @pl.when(block_z(t) // 4 == yl)
                def _():
                    keep(t).wait()

                @pl.when(block_z(t) // 4 != yl)
                def _():
                    out_copy(t, 0, 0).wait_send()


def lay_out(parts, out, held, laid, in_sem, out_sem):
    rows = laid.shape[2]
    half = rows // 2
    loads, stores = [], []
    for i in range(4):
        column, low = i // 2, i % 2 * 4
        for side in range(2):
            loads.append(pltpu.make_async_copy(
                parts.at[column, pl.ds(side * 8 + low, 4)], held.at[i, side], in_sem.at[i, side]))
            loads[-1].start()
        stores.append(pltpu.make_async_copy(
            laid.at[i], out.at[:, :, pl.ds(i * 4 * rows, 4 * rows)], out_sem.at[i]))
    for i in range(4):
        with scope("held"):
            loads[2 * i].wait()
            loads[2 * i + 1].wait()
        for b in range(4):
            block = held[i, 0, b].astype(F32) + held[i, 1, b].astype(F32)
            for part in range(2):
                for side in range(2):
                    at = (side * 2 + part) * rows
                    laid[i, part, side * half:side * half + half, b * rows:b * rows + rows] = block[:, at:at + rows]
        stores[i].start()
    with scope("stored"):
        for store in stores:
            store.wait()


def on_device(elements, screened, energies, freq_points, freq_weights, band_of_slot):
    slots = elements.shape[1]
    half = slots // 2
    anywhere = pl.BlockSpec(memory_space=pl.ANY)
    dma = pltpu.SemaphoreType.DMA
    parts = pl.pallas_call(
        kernel,
        out_shape=jax.ShapeDtypeStruct((2, 16, half, 4 * slots), BF16),
        in_specs=[anywhere] * 6,
        out_specs=anywhere,
        scratch_shapes=[
            pltpu.VMEM((4, 2, slots, 512), BF16),
            pltpu.VMEM((2, 8, slots, 512), BF16),
            pltpu.VMEM((4, 2, 2, 512, 512), BF16),
            pltpu.VMEM((4, 2 * slots, 512), F32),
            pltpu.VMEM((2, 8, 2, slots, 512), BF16),
            pltpu.VMEM((2, 2, slots, 512), BF16),
            pltpu.VMEM((2, 8, half, 4 * slots), F32),
            pltpu.VMEM((8, 8, half, 4 * slots), BF16),
            pltpu.VMEM((8, 8, half, 4 * slots), BF16),
            pltpu.VMEM((8, 8, half, 4 * slots), BF16),
            pltpu.VMEM((2, 16, slots, 128), F32),
            pltpu.VMEM((2, 8, 8, 2 * slots), F32),
            pltpu.VMEM((48, 128), F32),
            pltpu.VMEM((48, 128), jnp.int32),
            pltpu.VMEM((4, 16, 128), jnp.int32),
            pltpu.SMEM((2,), F32), pltpu.SMEM((2,), F32),
            dma((10,)), dma((8,)), dma((5,)), dma((5,)), dma, dma,
            dma((2, 2, 2)), dma((2, 2, 2)), dma((2, 4, 2)), dma((2, 4, 2)),
            dma((8,)), dma((8,)), dma((8, 8)), dma((2, 16)),
        ],
        compiler_params=pltpu.CompilerParams(
            collective_id=0, has_side_effects=True, vmem_limit_bytes=60 * 1024 * 1024),
        name="self_energy",
    )(elements, screened, energies.reshape(48, 128), band_of_slot.reshape(48, 128), freq_points, freq_weights)
    return pl.pallas_call(
        lay_out,
        out_shape=jax.ShapeDtypeStruct((2, slots, 16 * slots), F32),
        in_specs=[anywhere],
        out_specs=anywhere,
        scratch_shapes=[
            pltpu.VMEM((4, 2, 4, half, 4 * slots), BF16),
            pltpu.VMEM((4, 2, slots, 4 * slots), F32),
            dma((4, 2)), dma((4,)),
        ],
        compiler_params=pltpu.CompilerParams(vmem_limit_bytes=60 * 1024 * 1024),
        name="lay_out",
    )(parts)


def solution(mesh):
    torus = Mesh(mesh.devices.reshape(8, 2, 4, 2, 2), ("z", "yh", "x", "yl", "c"))
    return jax.shard_map(
        on_device,
        mesh=torus,
        in_specs=(P(None, BAND, GA), P(None, None, GA, None), P(), P(), P(), P()),
        out_specs=P(None, BAND, GA),
        check_vma=False,
    )
```

```python
import jax
import jax.numpy as jnp
from jax import lax
from jax.experimental import pallas as pl
from jax.experimental.pallas import tpu as pltpu
from jax.sharding import Mesh
from jax.sharding import PartitionSpec as P

BAND = ("z", "yh", "x")
GA = ("yl", "c")
F32 = jnp.float32
BF16 = jnp.bfloat16
scope = jax.named_scope


def dot_t(a, b):
    return lax.dot_general(a, b, (((1,), (1,)), ((), ())), preferred_element_type=F32)


def kernel(
    elements, screened, energies, bands, points, weights, o_recv,
    e_full, e_plane, w_buf, acc, y_buf, y_swap, s_sum, x_send, x_recv, h_send, h_recv, h_keep, o_buf, last_buf, s_col, s_row,
    energy_buf, band_buf, band_table, point_buf, weight_buf,
    load_sem, p_send, p_recv, a_recv, xr_send, xr_recv, z_send, z_recv,
    d_send, d_recv, hs_send, hs_recv, keep_sem, o_send, o_sem, last_send, last_sem,
):
    z, yh, x, yl, c = (lax.axis_index(name) for name in ("z", "yh", "x", "yl", "c"))
    own_q = yl * 2 + c
    own_b = yh * 4 + x
    slots = e_full.shape[2]

    def remote(src, dst, send, recv, **device):
        return pltpu.make_async_remote_copy(
            src_ref=src, dst_ref=dst, send_sem=send, recv_sem=recv,
            device_id=device, device_id_type=pl.DeviceIdType.MESH)

    quarter = [own_q, yl * 2 + (1 - c), (1 - yl) * 2 + c, (1 - yl) * 2 + (1 - c)]
    load_e = pltpu.make_async_copy(elements, e_full.at[own_q], load_sem.at[0])
    load_p = pltpu.make_async_copy(elements, e_plane.at[:, own_b], load_sem.at[1])
    load_e.start()
    load_p.start()
    load_s = [pltpu.make_async_copy(src, dst, load_sem.at[6 + i]) for i, (src, dst) in enumerate(
        ((energies, energy_buf), (bands, band_buf), (points, point_buf), (weights, weight_buf)))]
    load_w = []
    for k in range(4):
        at = pl.multiple_of(quarter[k] * 512, 512)
        load_w.append(pltpu.make_async_copy(screened.at[:, :, :, pl.ds(at, 512)], w_buf.at[k], load_sem.at[2 + k]))
        load_w[k].start()
    for load in load_s:
        load.start()

    barrier = pltpu.get_barrier_semaphore()

    def greet(**device):
        pl.semaphore_signal(barrier, inc=1, device_id=device, device_id_type=pl.DeviceIdType.MESH)

    def plane(dyh, dx, dyl):
        return dict(yh=lax.rem(yh + dyh, 2), x=lax.rem(x + dx, 4), yl=lax.rem(yl + dyl, 2))

    greet(c=1 - c)
    z_up, z_down = lax.rem(z + 1, 8), lax.rem(z + 7, 8)
    greet(z=z_up)
    greet(z=z_down)
    greet(yl=1 - yl)
    greet(yh=1 - yh, yl=1 - yl)
    greet(x=lax.rem(x + 1, 4))
    greet(x=lax.rem(x + 3, 4))
    with scope("enter"):
        pl.semaphore_wait(barrier, 7)
        load_e.wait()

    def to_y(h):
        ref = e_full.at[own_q, :, :, pl.ds(h * 256, 256)]
        return remote(ref, ref, p_send, p_recv.at[2 * h], yl=1 - yl)

    to_c = remote(e_full.at[own_q], e_full.at[own_q], p_send, p_recv.at[4], c=1 - c)
    to_y(0).start()
    to_y(1).start()
    to_c.start()
    load_p.wait()

    x_up, x_down = lax.rem(x + 1, 4), lax.rem(x + 3, 4)

    def block_at(k, at_x):
        return (yh if k == 0 else 1 - yh) * 4 + at_x

    def x_copy(k, way, hop):
        ahead, behind = (x_up, x_down) if way == 0 else (x_down, x_up)
        if hop == 1:
            ref = e_plane.at[:, block_at(k, x)]
        else:
            ref = e_plane.at[way, block_at(k, behind)]
        return remote(ref, ref, xr_send, xr_recv.at[k, way, hop - 1], x=ahead)

    for way in range(2):
        x_copy(0, way, 1).start()

    def terms(k, w, part, low, size):
        lhs = e_full[quarter[k], :, :, low:low + size].reshape(2 * slots, size)
        return dot_t(lhs, w_buf[k, w, part, :, low:low + size])

    def accumulate(k, low=0, size=512):
        for i in range(4):
            term = terms(k, i // 2, i % 2, low, size)
            acc[i] = term if k == 0 else acc[i] + term

    with scope("quarter0"):
        load_w[0].wait()
        accumulate(0)

    with scope("quarter1"):
        to_c.wait_recv()
        load_w[1].wait()
        accumulate(1)

    def pass_c(h):
        ref = e_full.at[quarter[2], :, :, pl.ds(h * 256, 256)]
        return remote(ref, ref, p_send, p_recv.at[2 * h + 1], c=1 - c)

    other = e_full.at[quarter[2]]
    to_a = remote(other, e_plane.at[:, own_b], p_send, a_recv, yh=1 - yh, yl=1 - yl)
    load_w[2].wait()
    load_w[3].wait()
    with scope("wait_y0"):
        to_y(0).wait_recv()
    pass_c(0).start()
    with scope("quarter2"):
        accumulate(2, 0, 256)
    with scope("wait_y1"):
        to_y(1).wait_recv()
    pass_c(1).start()
    to_a.start()
    with scope("quarter3"):
        accumulate(2, 256, 256)
        pass_c(0).wait_recv()
        accumulate(3, 0, 256)
    with scope("wait_c"):
        pass_c(1).wait_recv()

    def z_copy(way, hop, w):
        ahead = z_up if way == 0 else z_down
        owner = lax.rem(z + 8 - (hop - 1), 8) if way == 0 else lax.rem(z + hop - 1, 8)
        ref = y_buf.at[w, owner]
        return remote(ref, ref, z_send, z_recv.at[way, hop - 1, w], z=ahead)

    with scope("applied"):
        for w in range(2):
            real = acc[2 * w] + terms(3, w, 0, 256, 256)
            imag = acc[2 * w + 1] + terms(3, w, 1, 256, 256)
            y_buf[w, z, 0] = (real[:slots] - imag[slots:]).astype(BF16)
            y_buf[w, z, 1] = (imag[:slots] + real[slots:]).astype(BF16)
            if w == 0:
                z_copy(0, 1, 0).start()
        z_copy(1, 1, 1).start()
        z_copy(0, 1, 1).start()
        z_copy(1, 1, 0).start()

    def z_pass(hop, turn):
        for way in range(2):
            w = turn if way == 0 else 1 - turn
            z_copy(way, hop, w).wait_recv()
            if hop < 3 or (hop == 3 and turn == 0):
                z_copy(way, hop + 1, w).start()

    def x_pass(k):
        for way in range(2):
            x_copy(k, way, 1).wait_recv()
            x_copy(k, way, 2).start()

    def spread_bands():
        rows = [band_buf[pl.ds(k, 16, stride=3), :] for k in range(3)]
        band_table[0] = rows[0]
        band_table[1] = jnp.concatenate([rows[0][:, 96:], rows[1][:, :96]], axis=1)
        band_table[2] = jnp.concatenate([rows[1][:, 64:], rows[2][:, :64]], axis=1)
        band_table[3] = jnp.concatenate([rows[2][:, 32:], rows[2][:, :32]], axis=1)

    def look_up(i, carry):
        at = jnp.where(i < 8, z * 8 + i, (i - 8) * 8 + own_b)
        band = band_table[lax.rem(at, 4), pl.ds(at // 4, 1), :]
        band = jnp.broadcast_to(band, (128, 128)).T[:slots]
        lane = lax.broadcasted_iota(jnp.int32, (slots, 128), 1)

        def part(j, total):
            for u in range(8):
                row = j * 8 + u
                e = jnp.broadcast_to(energy_buf[pl.ds(row, 1), :], (slots, 128))
                total = total + jnp.where(band == lane + row * 128, e, 0.0)
            return total

        total = lax.fori_loop(0, 6, part, jnp.zeros((slots, 128), F32))
        energy = jnp.broadcast_to(jnp.sum(total, axis=1, keepdims=True), (slots, 128))
        for w in range(2):
            offset = energy - point_buf[w]
            s_col[w, i] = weight_buf[w] / (1.0 + 4.0 * offset * offset)
        return carry

    def turn(i, carry):
        w, g = i // 8, lax.rem(i, 8)
        one = s_col[w, 8 + g]
        s_row[w, g] = jnp.concatenate([one, one], axis=0).T[0:8]
        return carry

    with scope("x_pass0"):
        x_pass(0)
    with scope("look_up0"):
        for load in load_s:
            load.wait()
        spread_bands()
        lax.fori_loop(0, 8, look_up, 0)
    with scope("wait_a"):
        remote(other, e_plane.at[:, own_b], p_send, a_recv, yh=1 - yh, yl=1 - yl).wait_recv()
    for way in range(2):
        x_copy(1, way, 1).start()
    with scope("z10"):
        z_pass(1, 0)
    with scope("look_up1"):
        lax.fori_loop(8, 16, look_up, 0)
    with scope("x_pass1"):
        x_pass(1)
    with scope("z11"):
        z_pass(1, 1)
    with scope("turn"):
        lax.fori_loop(0, 16, turn, 0)
    with scope("z20"):
        z_pass(2, 0)
    with scope("wait_x"):
        for k in range(2):
            for way in range(2):
                x_copy(k, way, 2).wait_recv()

    half = slots // 2
    deltas = (0, 7, 1, 6, 2, 5, 3, 4)

    def block_z(t):
        return lax.rem(z + deltas[t], 8)

    def mine(t):
        return lax.rem(block_z(t) // 2, 2) == c

    def across(t):
        return remote(x_send.at[t], x_recv.at[t], d_send, d_recv.at[t], c=1 - c)

    @scope("products")
    def products(t):
        zz = block_z(t)
        for w in range(2):
            y_swap[w, 0] = y_buf[w, zz, 1]
            y_swap[w, 1] = -y_buf[w, zz, 0]
        for i in range(2):
            real = e_plane[0, i * 4:i * 4 + 4].reshape(4 * slots, 512)
            imag = e_plane[1, i * 4:i * 4 + 4].reshape(4 * slots, 512)
            total = None
            for w in range(2):
                both = dot_t(real, y_buf[w, zz].reshape(2 * slots, 512)) + dot_t(imag, y_swap[w].reshape(2 * slots, 512))
                s = s_col[w, i * 4:i * 4 + 4].reshape(4 * slots, 128)
                factor = 0.5 * (jnp.concatenate([s, s[:, :2 * slots - 128]], axis=1) + s_row[w, zz][0:1])
                total = both * factor if total is None else total + both * factor
            total = total.reshape(4, slots, 2 * slots)
            s_sum[t % 2, i * 4:i * 4 + 4] = jnp.concatenate([total[:, :half], total[:, half:]], axis=2)

        @pl.when(jnp.logical_not(mine(t)))
        def _():
            x_send[t] = s_sum[t % 2].astype(BF16)
            across(t).start()

    def same_yl(t):
        return block_z(t) // 4 == yl

    def rows_of(t):
        return jnp.where(same_yl(t), yh, 1 - yh)

    def partner(t):
        return remote(h_send.at[t], h_recv.at[t], hs_send, hs_recv.at[t], yl=1 - yl)

    @scope("reduce")
    def reduce(t):
        @pl.when(mine(t))
        def _():
            across(t).wait_recv()
            here = rows_of(t) * 4
            there = 4 - here
            h_send[t] = (s_sum[t % 2, pl.ds(there, 4)] + x_recv[t, pl.ds(there, 4)].astype(F32)).astype(BF16)
            partner(t).start()
            h_keep[t % 2] = s_sum[t % 2, pl.ds(here, 4)] + x_recv[t, pl.ds(here, 4)].astype(F32)

    def out_copy(t, dx):
        to_x = lax.rem(x + dx, 4)
        return remote(o_buf.at[t * 4 + to_x], o_recv.at[lax.rem(block_z(t), 2) * 16 + own_b], o_send, o_sem,
                      x=to_x, yh=rows_of(t), yl=jnp.where(same_yl(t), yl, 1 - yl))

    def keep(src, t):
        return pltpu.make_async_copy(src, o_recv.at[lax.rem(block_z(t), 2) * 16 + own_b], keep_sem)

    @scope("complete")
    def complete(t):
        @pl.when(mine(t))
        def _():
            partner(t).wait_recv()
            o_buf[t * 4:t * 4 + 4] = (h_keep[t % 2] + h_recv[t].astype(F32)).astype(BF16)
            for dx in (2, 1, 3):
                out_copy(t, dx).start()

            @pl.when(same_yl(t))
            def _():
                keep(o_buf.at[t * 4 + x], t).start()

            @pl.when(jnp.logical_not(same_yl(t)))
            def _():
                out_copy(t, 0).start()

    last = len(deltas) - 1

    def last_copy(dyh, dx, same):
        to_yh, to_x = lax.rem(yh + dyh, 2), lax.rem(x + dx, 4)
        index = lax.rem(block_z(last), 2) * 16 + own_b + (0 if same else 8)
        return remote(last_buf.at[to_yh * 4 + to_x], o_recv.at[index], last_send, last_sem.at[0 if same else 1],
                      yh=to_yh, x=to_x, yl=yl if same else 1 - yl)

    @scope("finish")
    def finish():
        @pl.when(mine(last))
        def _():
            across(last).wait_recv()
            last_buf[...] = (s_sum[last % 2] + x_recv[last].astype(F32)).astype(BF16)
            for same in (True, False):
                @pl.when(same_yl(last) == same)
                def _():
                    for dx in (2, 1, 3, 0):
                        for dyh in (1, 0):
                            if dx or dyh or not same:
                                last_copy(dyh, dx, same).start()
                    if same:
                        keep(last_buf.at[own_b], last).start()

    products(0)
    products(1)
    reduce(0)
    reduce(1)
    with scope("z21"):
        z_pass(2, 1)
    products(2)
    complete(0)
    complete(1)
    reduce(2)
    with scope("z30"):
        z_pass(3, 0)
    products(3)
    products(4)
    complete(2)
    reduce(3)
    reduce(4)
    with scope("z31"):
        z_pass(3, 1)
    products(5)
    products(6)
    complete(3)
    complete(4)
    reduce(5)
    reduce(6)
    with scope("z40"):
        z_pass(4, 0)
    products(7)
    finish()
    complete(5)
    complete(6)

    def drain(ref, sem):
        remote(ref, ref, sem, sem, c=1 - c).wait_send()

    with scope("wait_out"):
        drain(e_full, p_send)
        drain(e_plane.at[:, 0:6], xr_send)
        drain(y_buf.at[:, 0:7], z_send)
        drain(x_send.at[0:4], d_send)
        keep(o_buf.at[0], 0).wait()
        keep(o_buf.at[0], 0).wait()

        @pl.when(jnp.logical_not(mine(last)))
        def _():
            drain(h_send.at[0:4], hs_send)
            drain(o_buf.at[0:14], o_send)

        @pl.when(mine(last))
        def _():
            drain(h_send.at[0:3], hs_send)
            for same in (True, False):
                @pl.when(same_yl(last) == same)
                def _():
                    drain(o_buf.at[0:11 if same else 10], o_send)
                    drain(last_buf.at[0:7 if same else 8], last_send)

        drain_in = lambda n, sem: remote(o_recv.at[0:n], o_recv.at[0:n], o_send, sem, c=1 - c).wait_recv()
        has_last = block_z(last) // 2 == own_q

        @pl.when(jnp.logical_not(has_last))
        def _():
            drain_in(14, o_sem)

        @pl.when(has_last)
        def _():
            drain_in(7, o_sem)
            drain_in(7, last_sem.at[0])
            drain_in(8, last_sem.at[1])


def lay_out(parts, out, held, laid, in_sem, out_sem):
    rows = laid.shape[2]
    half = rows // 2
    stores = []
    def split(i):
        mine = (lax.axis_index("yl") * 2 + lax.axis_index("c")) * 2 + i // 2
        return mine == lax.rem(lax.axis_index("z") + 4, 8)

    def load(i, side):
        at = i // 2 * 16 + side * 8 + i % 2 * 4
        return pltpu.make_async_copy(parts.at[pl.ds(at, 4)], held.at[i, side], in_sem.at[i, side])

    for i in range(4):
        load(i, 0).start()

        @pl.when(split(i))
        def _():
            load(i, 1).start()

        stores.append(pltpu.make_async_copy(laid.at[i], out.at[:, :, pl.ds(i * 4 * rows, 4 * rows)], out_sem.at[i]))

    def place(i, both):
        for b in range(4):
            block = held[i, 0, b].astype(F32)
            if both:
                block = block + held[i, 1, b].astype(F32)
            for part in range(2):
                for side in range(2):
                    at = (side * 2 + part) * rows
                    laid[i, part, side * half:side * half + half, b * rows:b * rows + rows] = block[:, at:at + rows]

    for i in range(4):
        load(i, 0).wait()

        @pl.when(split(i))
        def _():
            load(i, 1).wait()
            place(i, True)

        @pl.when(jnp.logical_not(split(i)))
        def _():
            place(i, False)

        stores[i].start()
    for store in stores:
            store.wait()


def on_device(elements, screened, energies, freq_points, freq_weights, band_of_slot):
    slots = elements.shape[1]
    half = slots // 2
    anywhere = pl.BlockSpec(memory_space=pl.ANY)
    dma = pltpu.SemaphoreType.DMA
    parts = pl.pallas_call(
        kernel,
        out_shape=jax.ShapeDtypeStruct((32, half, 4 * slots), BF16),
        in_specs=[anywhere] * 6,
        out_specs=anywhere,
        scratch_shapes=[
            pltpu.VMEM((4, 2, slots, 512), BF16),
            pltpu.VMEM((2, 8, slots, 512), BF16),
            pltpu.VMEM((4, 2, 2, 512, 512), BF16),
            pltpu.VMEM((4, 2 * slots, 512), F32),
            pltpu.VMEM((2, 8, 2, slots, 512), BF16),
            pltpu.VMEM((2, 2, slots, 512), BF16),
            pltpu.VMEM((2, 8, half, 4 * slots), F32),
            pltpu.VMEM((8, 8, half, 4 * slots), BF16),
            pltpu.VMEM((8, 8, half, 4 * slots), BF16),
            pltpu.VMEM((8, 4, half, 4 * slots), BF16),
            pltpu.VMEM((8, 4, half, 4 * slots), BF16),
            pltpu.VMEM((2, 4, half, 4 * slots), F32),
            pltpu.VMEM((32, half, 4 * slots), BF16),
            pltpu.VMEM((8, half, 4 * slots), BF16),
            pltpu.VMEM((2, 16, slots, 128), F32),
            pltpu.VMEM((2, 8, 8, 2 * slots), F32),
            pltpu.VMEM((48, 128), F32),
            pltpu.VMEM((48, 128), jnp.int32),
            pltpu.VMEM((4, 16, 128), jnp.int32),
            pltpu.SMEM((2,), F32), pltpu.SMEM((2,), F32),
            dma((10,)), dma, dma((5,)), dma, dma, dma((2, 2, 2)), dma, dma((2, 4, 2)),
            dma, dma((8,)), dma, dma((8,)), dma, dma, dma, dma, dma((2,)),
        ],
        compiler_params=pltpu.CompilerParams(
            collective_id=0, has_side_effects=True, vmem_limit_bytes=60 * 1024 * 1024),
        name="self_energy",
    )(elements, screened, energies.reshape(48, 128), band_of_slot.reshape(48, 128), freq_points, freq_weights)
    return pl.pallas_call(
        lay_out,
        out_shape=jax.ShapeDtypeStruct((2, slots, 16 * slots), F32),
        in_specs=[anywhere],
        out_specs=anywhere,
        scratch_shapes=[
            pltpu.VMEM((4, 2, 4, half, 4 * slots), BF16),
            pltpu.VMEM((4, 2, slots, 4 * slots), F32),
            dma((4, 2)), dma((4,)),
        ],
        compiler_params=pltpu.CompilerParams(vmem_limit_bytes=60 * 1024 * 1024),
        name="lay_out",
    )(parts)


def solution(mesh):
    torus = Mesh(mesh.devices.reshape(8, 2, 4, 2, 2), ("z", "yh", "x", "yl", "c"))
    return jax.shard_map(
        on_device,
        mesh=torus,
        in_specs=(P(None, BAND, GA), P(None, None, GA, None), P(), P(), P(), P()),
        out_specs=P(None, BAND, GA),
        check_vma=False,
    )
```

```python
import jax
import jax.numpy as jnp
from jax import lax
from jax.experimental import pallas as pl
from jax.experimental.pallas import tpu as pltpu
from jax.sharding import Mesh
from jax.sharding import PartitionSpec as P

BAND = ("z", "yh", "x")
GA = ("yl", "c")
F32 = jnp.float32
BF16 = jnp.bfloat16
scope = jax.named_scope


def dot_t(a, b):
    return lax.dot_general(a, b, (((1,), (1,)), ((), ())), preferred_element_type=F32)


def kernel(
    elements, screened, energies, bands, points, weights, o_recv,
    e_full, e_ring, e_plane, w_buf, acc, acc_near, y_buf, y_swap, s_sum, x_send, x_recv, h_send, h_recv, h_keep, o_buf, last_buf, s_col, s_row,
    energy_buf, band_buf, band_table, point_buf, weight_buf,
    load_sem, p_send, p_recv, a_recv, xr_send, xr_recv, er_send, er_recv, share_recv, s_send, s_recv, z_send, z_recv,
    d_send, d_recv, hs_send, hs_recv, keep_sem, o_send, o_sem, last_send, last_sem,
):
    z, yh, x, yl, c = (lax.axis_index(name) for name in ("z", "yh", "x", "yl", "c"))
    own_q = yl * 2 + c
    own_b = yh * 4 + x
    slots = e_full.shape[2]

    def remote(src, dst, send, recv, **device):
        return pltpu.make_async_remote_copy(
            src_ref=src, dst_ref=dst, send_sem=send, recv_sem=recv,
            device_id=device, device_id_type=pl.DeviceIdType.MESH)

    quarter = [own_q, yl * 2 + (1 - c), (1 - yl) * 2 + c, (1 - yl) * 2 + (1 - c)]
    load_e = pltpu.make_async_copy(elements, e_full.at[own_q], load_sem.at[0])
    load_p = pltpu.make_async_copy(elements, e_plane.at[:, own_b], load_sem.at[1])
    load_e.start()
    load_p.start()
    load_s = [pltpu.make_async_copy(src, dst, load_sem.at[6 + i]) for i, (src, dst) in enumerate(
        ((energies, energy_buf), (bands, band_buf), (points, point_buf), (weights, weight_buf)))]
    load_w = []
    for k in range(4):
        at = pl.multiple_of(quarter[k] * 512, 512)
        load_w.append(pltpu.make_async_copy(screened.at[:, :, :, pl.ds(at, 512)], w_buf.at[k], load_sem.at[2 + k]))
        load_w[k].start()
    for load in load_s:
        load.start()

    barrier = pltpu.get_barrier_semaphore()

    def greet(**device):
        pl.semaphore_signal(barrier, inc=1, device_id=device, device_id_type=pl.DeviceIdType.MESH)

    def plane(dyh, dx, dyl):
        return dict(yh=lax.rem(yh + dyh, 2), x=lax.rem(x + dx, 4), yl=lax.rem(yl + dyl, 2))

    greet(c=1 - c)
    z_up, z_down = lax.rem(z + 1, 8), lax.rem(z + 7, 8)
    greet(z=z_up)
    greet(z=z_down)
    greet(yl=1 - yl)
    greet(yh=1 - yh, yl=1 - yl)
    greet(x=lax.rem(x + 1, 4))
    greet(x=lax.rem(x + 3, 4))
    with scope("enter"):
        pl.semaphore_wait(barrier, 7)
        load_e.wait()

    def to_y(h):
        ref = e_full.at[own_q, :, :, pl.ds(h * 256, 256)]
        return remote(ref, ref, p_send, p_recv.at[2 * h], yl=1 - yl)

    to_c = remote(e_full.at[own_q], e_full.at[own_q], p_send, p_recv.at[4], c=1 - c)
    to_y(0).start()
    to_y(1).start()
    to_c.start()
    load_p.wait()

    x_up, x_down = lax.rem(x + 1, 4), lax.rem(x + 3, 4)

    def block_at(k, at_x):
        return (yh if k == 0 else 1 - yh) * 4 + at_x

    def x_copy(k, way, hop):
        ahead, behind = (x_up, x_down) if way == 0 else (x_down, x_up)
        if hop == 1:
            ref = e_plane.at[:, block_at(k, x)]
        else:
            ref = e_plane.at[way, block_at(k, behind)]
        return remote(ref, ref, xr_send, xr_recv.at[k, way, hop - 1], x=ahead)

    def piece_of(ref, piece):
        if piece == 0:
            return ref.at[own_q]
        return ref.at[quarter[2], :, :, pl.ds((piece - 1) * 256, 256)]

    def ring(way, hop, piece):
        src = piece_of(e_full if hop == 1 else e_ring.at[way], piece)
        dst = piece_of(e_ring.at[way + 2 * hop - 2], piece)
        return remote(src, dst, er_send, er_recv.at[way, hop - 1, piece], z=z_up if way == 0 else z_down)

    def share(slot, piece):
        ref = piece_of(e_ring.at[slot], piece)
        return remote(ref, ref, er_send, share_recv.at[slot, piece], c=1 - c)

    def ring_start(piece):
        for way in range(2):
            ring(way, 1, piece).start()

    def ring_pass(hop, piece):
        for way in range(2):
            ring(way, hop, piece).wait_recv()
            if hop == 1:
                ring(way, 2, piece).start()
            share(way + 2 * hop - 2, piece).start()

    def shared(hop, piece):
        for way in range(2):
            share(way + 2 * hop - 2, piece).wait_recv()

    ring_start(0)
    for way in range(2):
        x_copy(0, way, 1).start()

    def spread_bands():
        rows = [band_buf[pl.ds(k, 16, stride=3), :] for k in range(3)]
        band_table[0] = rows[0]
        band_table[1] = jnp.concatenate([rows[0][:, 96:], rows[1][:, :96]], axis=1)
        band_table[2] = jnp.concatenate([rows[1][:, 64:], rows[2][:, :64]], axis=1)
        band_table[3] = jnp.concatenate([rows[2][:, 32:], rows[2][:, :32]], axis=1)

    def look_up(i, carry):
        i = i + c * 8
        at = jnp.where(i < 8, z * 8 + i, (i - 8) * 8 + own_b)
        band = band_table[lax.rem(at, 4), pl.ds(at // 4, 1), :]
        band = jnp.broadcast_to(band, (128, 128)).T[:slots]
        lane = lax.broadcasted_iota(jnp.int32, (slots, 128), 1)

        def part(j, total):
            for u in range(8):
                row = j * 8 + u
                e = jnp.broadcast_to(energy_buf[pl.ds(row, 1), :], (slots, 128))
                total = total + jnp.where(band == lane + row * 128, e, 0.0)
            return total

        total = lax.fori_loop(0, 6, part, jnp.zeros((slots, 128), F32))
        energy = jnp.broadcast_to(jnp.sum(total, axis=1, keepdims=True), (slots, 128))
        for w in range(2):
            offset = energy - point_buf[w]
            s_col[w, i] = weight_buf[w] / (1.0 + 4.0 * offset * offset)
        return carry

    def turn(i, carry):
        w, g = i // 8, lax.rem(i, 8)
        one = s_col[w, 8 + g]
        s_row[w, g] = jnp.concatenate([one, one], axis=0).T[0:8]
        return carry

    def look_up_some(n, m):
        with scope("look_up"):
            lax.fori_loop(n, m, look_up, 0)

    def terms(k, w, part, low, size):
        lhs = e_full[quarter[k], :, :, low:low + size].reshape(2 * slots, size)
        return dot_t(lhs, w_buf[k, w, part, :, low:low + size])

    def accumulate(k, low=0, size=512):
        for i in range(4):
            term = terms(k, i // 2, i % 2, low, size)
            acc[i] = term if k == 0 else acc[i] + term

    with scope("quarter0"):
        load_w[0].wait()
        accumulate(0)

    with scope("quarter1"):
        to_c.wait_recv()
        load_w[1].wait()
        accumulate(1)

    def pass_c(h):
        ref = e_full.at[quarter[2], :, :, pl.ds(h * 256, 256)]
        return remote(ref, ref, p_send, p_recv.at[2 * h + 1], c=1 - c)

    other = e_full.at[quarter[2]]
    to_a = remote(other, e_plane.at[:, own_b], p_send, a_recv, yh=1 - yh, yl=1 - yl)
    load_w[2].wait()
    load_w[3].wait()
    for load in load_s:
        load.wait()
    spread_bands()
    look_up_some(0, 3)
    with scope("wait_y0"):
        to_y(0).wait_recv()
    pass_c(0).start()
    ring_start(1)
    with scope("quarter2"):
        accumulate(2, 0, 256)
    look_up_some(3, 5)
    with scope("quarter2b"):
        pass_c(0).wait_recv()
        accumulate(3, 0, 256)
    with scope("wait_y1"):
        to_y(1).wait_recv()
    pass_c(1).start()
    ring_start(2)
    to_a.start()
    with scope("quarter3"):
        accumulate(2, 256, 256)
    with scope("ring10"):
        ring_pass(1, 0)
    with scope("wait_c"):
        pass_c(1).wait_recv()

    def z_copy(way, hop, w):
        ahead = z_up if way == 0 else z_down
        owner = lax.rem(z + 8 - (hop - 1), 8) if way == 0 else lax.rem(z + hop - 1, 8)
        ref = y_buf.at[w, owner]
        return remote(ref, ref, z_send, z_recv.at[way, hop - 3, w], z=ahead)

    def z_pass(hop, turn):
        for way in range(2):
            w = turn if way == 0 else 1 - turn
            z_copy(way, hop, w).wait_recv()
            if hop == 3 and turn == 0:
                z_copy(way, 4, w).start()

    def apply_to(w, zz, real, imag, low):
        y_buf[w, zz, 0] = (real[low:low + slots] - imag[low + slots:low + 2 * slots]).astype(BF16)
        y_buf[w, zz, 1] = (imag[low:low + slots] + real[low + slots:low + 2 * slots]).astype(BF16)

    with scope("applied"):
        for w in range(2):
            apply_to(w, z, acc[2 * w] + terms(3, w, 0, 256, 256), acc[2 * w + 1] + terms(3, w, 1, 256, 256), 0)

    def near_terms(hop, k, i):
        lhs = e_ring[2 * hop - 2:2 * hop, quarter[k]].reshape(4 * slots, 512)
        return dot_t(lhs, w_buf[k, i // 2, i % 2])

    @scope("near")
    def near(hop, k):
        for i in range(4):
            term = near_terms(hop, k, i)
            acc_near[i] = term if k == 0 else acc_near[i] + term

    @scope("near_applied")
    def near_applied(hop, w):
        real = acc_near[2 * w] + near_terms(hop, 3, 2 * w)
        imag = acc_near[2 * w + 1] + near_terms(hop, 3, 2 * w + 1)
        apply_to(w, lax.rem(z + 8 - hop, 8), real, imag, 0)
        apply_to(w, lax.rem(z + hop, 8), real, imag, 2 * slots)

    def x_pass(k):
        for way in range(2):
            x_copy(k, way, 1).wait_recv()
            x_copy(k, way, 2).start()

    def s_copy():
        ref = s_col.at[:, pl.ds(c * 8, 8)]
        return remote(ref, ref, s_send, s_recv, c=1 - c)

    with scope("x_pass0"):
        x_pass(0)
    look_up_some(5, 6)
    with scope("ring11"):
        ring_pass(1, 1)
    near(1, 0)
    with scope("shared10"):
        shared(1, 0)
    near(1, 1)
    with scope("ring12"):
        ring_pass(1, 2)
    look_up_some(6, 7)
    near(1, 2)
    with scope("wait_a"):
        remote(other, e_plane.at[:, own_b], p_send, a_recv, yh=1 - yh, yl=1 - yl).wait_recv()
    for way in range(2):
        x_copy(1, way, 1).start()
    with scope("shared11"):
        shared(1, 1)
        shared(1, 2)
    near_applied(1, 0)
    near_applied(1, 1)
    look_up_some(7, 8)
    s_copy().start()
    with scope("ring20"):
        ring_pass(2, 0)
    near(2, 0)
    with scope("ring21"):
        ring_pass(2, 1)
    with scope("shared20"):
        shared(2, 0)
    near(2, 1)
    with scope("x_pass1"):
        x_pass(1)
    with scope("ring22"):
        ring_pass(2, 2)
    near(2, 2)
    with scope("shared21"):
        shared(2, 1)
        shared(2, 2)
    near_applied(2, 0)
    z_copy(0, 3, 0).start()
    near_applied(2, 1)
    z_copy(1, 3, 1).start()
    z_copy(0, 3, 1).start()
    z_copy(1, 3, 0).start()
    with scope("turn"):
        s_copy().wait_recv()
        lax.fori_loop(0, 16, turn, 0)
    with scope("wait_x"):
        for k in range(2):
            for way in range(2):
                x_copy(k, way, 2).wait_recv()

    half = slots // 2
    deltas = (0, 7, 1, 6, 2, 5, 3, 4)

    def block_z(t):
        return lax.rem(z + deltas[t], 8)

    def mine(t):
        return lax.rem(block_z(t) // 2, 2) == c

    def across(t):
        return remote(x_send.at[t], x_recv.at[t], d_send, d_recv.at[t], c=1 - c)

    @scope("products")
    def products(t):
        zz = block_z(t)
        for w in range(2):
            y_swap[w, 0] = y_buf[w, zz, 1]
            y_swap[w, 1] = -y_buf[w, zz, 0]
        for i in range(2):
            real = e_plane[0, i * 4:i * 4 + 4].reshape(4 * slots, 512)
            imag = e_plane[1, i * 4:i * 4 + 4].reshape(4 * slots, 512)
            total = None
            for w in range(2):
                both = dot_t(real, y_buf[w, zz].reshape(2 * slots, 512)) + dot_t(imag, y_swap[w].reshape(2 * slots, 512))
                s = s_col[w, i * 4:i * 4 + 4].reshape(4 * slots, 128)
                factor = 0.5 * (jnp.concatenate([s, s[:, :2 * slots - 128]], axis=1) + s_row[w, zz][0:1])
                total = both * factor if total is None else total + both * factor
            total = total.reshape(4, slots, 2 * slots)
            s_sum[t % 2, i * 4:i * 4 + 4] = jnp.concatenate([total[:, :half], total[:, half:]], axis=2)

        @pl.when(jnp.logical_not(mine(t)))
        def _():
            x_send[t] = s_sum[t % 2].astype(BF16)
            across(t).start()

    def same_yl(t):
        return block_z(t) // 4 == yl

    def rows_of(t):
        return jnp.where(same_yl(t), yh, 1 - yh)

    def partner(t):
        return remote(h_send.at[t], h_recv.at[t], hs_send, hs_recv.at[t], yl=1 - yl)

    @scope("reduce")
    def reduce(t):
        @pl.when(mine(t))
        def _():
            across(t).wait_recv()
            here = rows_of(t) * 4
            there = 4 - here
            h_send[t] = (s_sum[t % 2, pl.ds(there, 4)] + x_recv[t, pl.ds(there, 4)].astype(F32)).astype(BF16)
            partner(t).start()
            h_keep[t] = s_sum[t % 2, pl.ds(here, 4)] + x_recv[t, pl.ds(here, 4)].astype(F32)

    def out_copy(t, dx):
        to_x = lax.rem(x + dx, 4)
        return remote(o_buf.at[t * 4 + to_x], o_recv.at[lax.rem(block_z(t), 2) * 16 + own_b], o_send, o_sem,
                      x=to_x, yh=rows_of(t), yl=jnp.where(same_yl(t), yl, 1 - yl))

    def keep(src, t):
        return pltpu.make_async_copy(src, o_recv.at[lax.rem(block_z(t), 2) * 16 + own_b], keep_sem)

    @scope("complete")
    def complete(t):
        @pl.when(mine(t))
        def _():
            partner(t).wait_recv()
            o_buf[t * 4:t * 4 + 4] = (h_keep[t] + h_recv[t].astype(F32)).astype(BF16)
            for dx in (2, 1, 3):
                out_copy(t, dx).start()

            @pl.when(same_yl(t))
            def _():
                keep(o_buf.at[t * 4 + x], t).start()

            @pl.when(jnp.logical_not(same_yl(t)))
            def _():
                out_copy(t, 0).start()

    last = len(deltas) - 1

    def last_copy(dyh, dx, same):
        to_yh, to_x = lax.rem(yh + dyh, 2), lax.rem(x + dx, 4)
        index = lax.rem(block_z(last), 2) * 16 + own_b + (0 if same else 8)
        return remote(last_buf.at[to_yh * 4 + to_x], o_recv.at[index], last_send, last_sem.at[0 if same else 1],
                      yh=to_yh, x=to_x, yl=yl if same else 1 - yl)

    @scope("finish")
    def finish():
        @pl.when(mine(last))
        def _():
            across(last).wait_recv()
            last_buf[...] = (s_sum[last % 2] + x_recv[last].astype(F32)).astype(BF16)
            for same in (True, False):
                @pl.when(same_yl(last) == same)
                def _():
                    for dx in (2, 1, 3, 0):
                        for dyh in (1, 0):
                            if dx or dyh or not same:
                                last_copy(dyh, dx, same).start()
                    if same:
                        keep(last_buf.at[own_b], last).start()

    products(0)
    products(1)
    reduce(0)
    products(2)
    reduce(1)
    products(3)
    reduce(2)
    with scope("z30"):
        z_pass(3, 0)
    products(4)
    reduce(3)
    complete(0)
    complete(1)
    reduce(4)
    complete(2)
    with scope("z31"):
        z_pass(3, 1)
    products(5)
    products(6)
    complete(3)
    complete(4)
    reduce(5)
    reduce(6)
    with scope("z40"):
        z_pass(4, 0)
    products(7)
    finish()
    complete(5)
    complete(6)

    def drain(ref, sem):
        remote(ref, ref, sem, sem, c=1 - c).wait_send()

    with scope("wait_out"):
        drain(e_full, p_send)
        drain(e_plane.at[:, 0:6], xr_send)
        drain(e_ring, er_send)
        s_copy().wait_send()
        drain(y_buf.at[:, 0:3], z_send)
        drain(x_send.at[0:4], d_send)
        keep(o_buf.at[0], 0).wait()
        keep(o_buf.at[0], 0).wait()

        @pl.when(jnp.logical_not(mine(last)))
        def _():
            drain(h_send.at[0:4], hs_send)
            drain(o_buf.at[0:14], o_send)

        @pl.when(mine(last))
        def _():
            drain(h_send.at[0:3], hs_send)
            for same in (True, False):
                @pl.when(same_yl(last) == same)
                def _():
                    drain(o_buf.at[0:11 if same else 10], o_send)
                    drain(last_buf.at[0:7 if same else 8], last_send)

        drain_in = lambda n, sem: remote(o_recv.at[0:n], o_recv.at[0:n], o_send, sem, c=1 - c).wait_recv()
        has_last = block_z(last) // 2 == own_q

        @pl.when(jnp.logical_not(has_last))
        def _():
            drain_in(14, o_sem)

        @pl.when(has_last)
        def _():
            drain_in(7, o_sem)
            drain_in(7, last_sem.at[0])
            drain_in(8, last_sem.at[1])


def lay_out(parts, out, held, laid, in_sem, out_sem):
    rows = laid.shape[2]
    half = rows // 2
    stores = []
    def split(i):
        mine = (lax.axis_index("yl") * 2 + lax.axis_index("c")) * 2 + i // 2
        return mine == lax.rem(lax.axis_index("z") + 4, 8)

    def load(i, side):
        at = i // 2 * 16 + side * 8 + i % 2 * 4
        return pltpu.make_async_copy(parts.at[pl.ds(at, 4)], held.at[i, side], in_sem.at[i, side])

    for i in range(4):
        load(i, 0).start()

        @pl.when(split(i))
        def _():
            load(i, 1).start()

        stores.append(pltpu.make_async_copy(laid.at[i], out.at[:, :, pl.ds(i * 4 * rows, 4 * rows)], out_sem.at[i]))

    def place(i, both):
        for b in range(4):
            block = held[i, 0, b].astype(F32)
            if both:
                block = block + held[i, 1, b].astype(F32)
            for part in range(2):
                for side in range(2):
                    at = (side * 2 + part) * rows
                    laid[i, part, side * half:side * half + half, b * rows:b * rows + rows] = block[:, at:at + rows]

    for i in range(4):
        load(i, 0).wait()

        @pl.when(split(i))
        def _():
            load(i, 1).wait()
            place(i, True)

        @pl.when(jnp.logical_not(split(i)))
        def _():
            place(i, False)

        stores[i].start()
    for store in stores:
            store.wait()


def on_device(elements, screened, energies, freq_points, freq_weights, band_of_slot):
    slots = elements.shape[1]
    half = slots // 2
    anywhere = pl.BlockSpec(memory_space=pl.ANY)
    dma = pltpu.SemaphoreType.DMA
    parts = pl.pallas_call(
        kernel,
        out_shape=jax.ShapeDtypeStruct((32, half, 4 * slots), BF16),
        in_specs=[anywhere] * 6,
        out_specs=anywhere,
        scratch_shapes=[
            pltpu.VMEM((4, 2, slots, 512), BF16),
            pltpu.VMEM((4, 4, 2, slots, 512), BF16),
            pltpu.VMEM((2, 8, slots, 512), BF16),
            pltpu.VMEM((4, 2, 2, 512, 512), BF16),
            pltpu.VMEM((4, 2 * slots, 512), F32),
            pltpu.VMEM((4, 4 * slots, 512), F32),
            pltpu.VMEM((2, 8, 2, slots, 512), BF16),
            pltpu.VMEM((2, 2, slots, 512), BF16),
            pltpu.VMEM((2, 8, half, 4 * slots), F32),
            pltpu.VMEM((8, 8, half, 4 * slots), BF16),
            pltpu.VMEM((8, 8, half, 4 * slots), BF16),
            pltpu.VMEM((8, 4, half, 4 * slots), BF16),
            pltpu.VMEM((8, 4, half, 4 * slots), BF16),
            pltpu.VMEM((8, 4, half, 4 * slots), F32),
            pltpu.VMEM((32, half, 4 * slots), BF16),
            pltpu.VMEM((8, half, 4 * slots), BF16),
            pltpu.VMEM((2, 16, slots, 128), F32),
            pltpu.VMEM((2, 8, 8, 2 * slots), F32),
            pltpu.VMEM((48, 128), F32),
            pltpu.VMEM((48, 128), jnp.int32),
            pltpu.VMEM((4, 16, 128), jnp.int32),
            pltpu.SMEM((2,), F32), pltpu.SMEM((2,), F32),
            dma((10,)), dma, dma((5,)), dma, dma, dma((2, 2, 2)),
            dma, dma((2, 2, 3)), dma((4, 3)), dma, dma, dma, dma((2, 2, 2)),
            dma, dma((8,)), dma, dma((8,)), dma, dma, dma, dma, dma((2,)),
        ],
        compiler_params=pltpu.CompilerParams(
            collective_id=0, has_side_effects=True, vmem_limit_bytes=60 * 1024 * 1024),
        name="self_energy",
    )(elements, screened, energies.reshape(48, 128), band_of_slot.reshape(48, 128), freq_points, freq_weights)
    return pl.pallas_call(
        lay_out,
        out_shape=jax.ShapeDtypeStruct((2, slots, 16 * slots), F32),
        in_specs=[anywhere],
        out_specs=anywhere,
        scratch_shapes=[
            pltpu.VMEM((4, 2, 4, half, 4 * slots), BF16),
            pltpu.VMEM((4, 2, slots, 4 * slots), F32),
            dma((4, 2)), dma((4,)),
        ],
        compiler_params=pltpu.CompilerParams(vmem_limit_bytes=60 * 1024 * 1024),
        name="lay_out",
    )(parts)


def solution(mesh):
    torus = Mesh(mesh.devices.reshape(8, 2, 4, 2, 2), ("z", "yh", "x", "yl", "c"))
    return jax.shard_map(
        on_device,
        mesh=torus,
        in_specs=(P(None, BAND, GA), P(None, None, GA, None), P(), P(), P(), P()),
        out_specs=P(None, BAND, GA),
        check_vma=False,
    )
```

```python
import jax
import jax.numpy as jnp
from jax import lax
from jax.experimental import pallas as pl
from jax.experimental.pallas import tpu as pltpu
from jax.sharding import Mesh
from jax.sharding import PartitionSpec as P

BAND = ("z", "yh", "x")
GA = ("yl", "c")
F32 = jnp.float32
BF16 = jnp.bfloat16
scope = jax.named_scope


def dot_t(a, b):
    return lax.dot_general(a, b, (((1,), (1,)), ((), ())), preferred_element_type=F32)


def kernel(
    elements, screened, energies, bands, points, weights, o_recv,
    e_full, e_ring, e_plane, w_buf, acc, acc_near, y_buf, y_swap, s_sum, x_send, x_recv, h_send, h_recv, h_keep, o_buf, last_buf, s_col, s_row,
    energy_buf, band_buf, band_table, point_buf, weight_buf,
    load_sem, p_send, p_recv, a_recv, xr_send, xr_recv, er_send, er_recv, share_recv, s_send, s_recv, z_send, z_recv,
    d_send, d_recv, hs_send, hs_recv, keep_sem, o_send, o_sem, last_send, last_sem,
):
    z, yh, x, yl, c = (lax.axis_index(name) for name in ("z", "yh", "x", "yl", "c"))
    own_q = yl * 2 + c
    own_b = yh * 4 + x
    slots = e_full.shape[2]

    def remote(src, dst, send, recv, **device):
        return pltpu.make_async_remote_copy(
            src_ref=src, dst_ref=dst, send_sem=send, recv_sem=recv,
            device_id=device, device_id_type=pl.DeviceIdType.MESH)

    quarter = [own_q, yl * 2 + (1 - c), (1 - yl) * 2 + c, (1 - yl) * 2 + (1 - c)]
    load_e = pltpu.make_async_copy(elements, e_full.at[own_q], load_sem.at[0])
    load_p = pltpu.make_async_copy(elements, e_plane.at[:, own_b], load_sem.at[1])
    load_e.start()
    load_p.start()
    load_s = [pltpu.make_async_copy(src, dst, load_sem.at[6 + i]) for i, (src, dst) in enumerate(
        ((energies, energy_buf), (bands, band_buf), (points, point_buf), (weights, weight_buf)))]
    load_w = []
    for k in range(4):
        at = pl.multiple_of(quarter[k] * 512, 512)
        load_w.append(pltpu.make_async_copy(screened.at[:, :, :, pl.ds(at, 512)], w_buf.at[k], load_sem.at[2 + k]))
        load_w[k].start()
    for load in load_s:
        load.start()

    barrier = pltpu.get_barrier_semaphore()

    def greet(**device):
        pl.semaphore_signal(barrier, inc=1, device_id=device, device_id_type=pl.DeviceIdType.MESH)

    def plane(dyh, dx, dyl):
        return dict(yh=lax.rem(yh + dyh, 2), x=lax.rem(x + dx, 4), yl=lax.rem(yl + dyl, 2))

    greet(c=1 - c)
    z_up, z_down = lax.rem(z + 1, 8), lax.rem(z + 7, 8)
    greet(z=z_up)
    greet(z=z_down)
    greet(yl=1 - yl)
    greet(yh=1 - yh, yl=1 - yl)
    greet(x=lax.rem(x + 1, 4))
    greet(x=lax.rem(x + 3, 4))
    with scope("enter"):
        pl.semaphore_wait(barrier, 7)
        load_e.wait()

    def to_y(h):
        ref = e_full.at[own_q, :, :, pl.ds(h * 256, 256)]
        return remote(ref, ref, p_send, p_recv.at[2 * h], yl=1 - yl)

    to_c = remote(e_full.at[own_q], e_full.at[own_q], p_send, p_recv.at[4], c=1 - c)
    to_y(0).start()
    to_y(1).start()
    to_c.start()
    load_p.wait()

    x_up, x_down = lax.rem(x + 1, 4), lax.rem(x + 3, 4)

    def block_at(k, at_x):
        return (yh if k == 0 else 1 - yh) * 4 + at_x

    def x_copy(k, way, hop):
        ahead, behind = (x_up, x_down) if way == 0 else (x_down, x_up)
        if hop == 1:
            ref = e_plane.at[:, block_at(k, x)]
        else:
            ref = e_plane.at[way, block_at(k, behind)]
        return remote(ref, ref, xr_send, xr_recv.at[k, way, hop - 1], x=ahead)

    def piece_of(ref, piece):
        if piece == 0:
            return ref.at[own_q]
        return ref.at[quarter[2], :, :, pl.ds((piece - 1) * 256, 256)]

    def ring(way, piece):
        return remote(piece_of(e_full, piece), piece_of(e_ring.at[way], piece), er_send, er_recv.at[way, piece],
                      z=z_up if way == 0 else z_down)

    def share(way, piece):
        ref = piece_of(e_ring.at[way], piece)
        return remote(ref, ref, er_send, share_recv.at[way, piece], c=1 - c)

    def ring_start(piece):
        for way in range(2):
            ring(way, piece).start()

    def ring_pass(piece):
        for way in range(2):
            ring(way, piece).wait_recv()
            share(way, piece).start()

    def shared(piece):
        for way in range(2):
            share(way, piece).wait_recv()

    ring_start(0)
    for way in range(2):
        x_copy(0, way, 1).start()

    def spread_bands():
        rows = [band_buf[pl.ds(k, 16, stride=3), :] for k in range(3)]
        band_table[0] = rows[0]
        band_table[1] = jnp.concatenate([rows[0][:, 96:], rows[1][:, :96]], axis=1)
        band_table[2] = jnp.concatenate([rows[1][:, 64:], rows[2][:, :64]], axis=1)
        band_table[3] = jnp.concatenate([rows[2][:, 32:], rows[2][:, :32]], axis=1)

    def look_up(i, carry):
        i = i + c * 8
        at = jnp.where(i < 8, z * 8 + i, (i - 8) * 8 + own_b)
        band = band_table[lax.rem(at, 4), pl.ds(at // 4, 1), :]
        band = jnp.broadcast_to(band, (128, 128)).T[:slots]
        lane = lax.broadcasted_iota(jnp.int32, (slots, 128), 1)

        def part(j, total):
            for u in range(8):
                row = j * 8 + u
                e = jnp.broadcast_to(energy_buf[pl.ds(row, 1), :], (slots, 128))
                total = total + jnp.where(band == lane + row * 128, e, 0.0)
            return total

        total = lax.fori_loop(0, 6, part, jnp.zeros((slots, 128), F32))
        energy = jnp.broadcast_to(jnp.sum(total, axis=1, keepdims=True), (slots, 128))
        for w in range(2):
            offset = energy - point_buf[w]
            s_col[w, i] = weight_buf[w] / (1.0 + 4.0 * offset * offset)
        return carry

    def turn(i, carry):
        w, g = i // 8, lax.rem(i, 8)
        one = s_col[w, 8 + g]
        s_row[w, g] = jnp.concatenate([one, one], axis=0).T[0:8]
        return carry

    def look_up_some(n, m):
        with scope("look_up"):
            lax.fori_loop(n, m, look_up, 0)

    def terms(k, w, part, low, size):
        lhs = e_full[quarter[k], :, :, low:low + size].reshape(2 * slots, size)
        return dot_t(lhs, w_buf[k, w, part, :, low:low + size])

    def accumulate(k, low=0, size=512):
        for i in range(4):
            term = terms(k, i // 2, i % 2, low, size)
            acc[i] = term if k == 0 else acc[i] + term

    with scope("quarter0"):
        load_w[0].wait()
        accumulate(0)

    with scope("quarter1"):
        to_c.wait_recv()
        load_w[1].wait()
        accumulate(1)

    def pass_c(h):
        ref = e_full.at[quarter[2], :, :, pl.ds(h * 256, 256)]
        return remote(ref, ref, p_send, p_recv.at[2 * h + 1], c=1 - c)

    other = e_full.at[quarter[2]]

    def to_a(h):
        cols = pl.ds(h * 256, 256)
        return remote(other.at[:, :, cols], e_plane.at[:, own_b, :, cols], p_send, a_recv.at[h], yh=1 - yh, yl=1 - yl)

    load_w[2].wait()
    load_w[3].wait()
    for load in load_s:
        load.wait()
    spread_bands()
    look_up_some(0, 3)
    with scope("wait_y0"):
        to_y(0).wait_recv()
    pass_c(0).start()
    ring_start(1)
    to_a(0).start()
    with scope("quarter2"):
        accumulate(2, 0, 256)
    look_up_some(3, 5)
    with scope("quarter2b"):
        pass_c(0).wait_recv()
        accumulate(3, 0, 256)
    with scope("wait_y1"):
        to_y(1).wait_recv()
    pass_c(1).start()
    ring_start(2)
    to_a(1).start()
    with scope("quarter3"):
        accumulate(2, 256, 256)

    def z_copy(way, hop, w):
        ahead = z_up if way == 0 else z_down
        owner = lax.rem(z + 8 - (hop - 1), 8) if way == 0 else lax.rem(z + hop - 1, 8)
        ref = y_buf.at[w, owner]
        return remote(ref, ref, z_send, z_recv.at[way, hop - 2, w], z=ahead)

    def z_pass(hop, turn):
        for way in range(2):
            w = turn if way == 0 else 1 - turn
            z_copy(way, hop, w).wait_recv()
            if hop == 2 or (hop == 3 and turn == 0):
                z_copy(way, hop + 1, w).start()

    def apply_to(w, zz, real, imag, low):
        y_buf[w, zz, 0] = (real[low:low + slots] - imag[low + slots:low + 2 * slots]).astype(BF16)
        y_buf[w, zz, 1] = (imag[low:low + slots] + real[low + slots:low + 2 * slots]).astype(BF16)

    @scope("applied")
    def applied():
        for w in range(2):
            apply_to(w, z, acc[2 * w] + terms(3, w, 0, 256, 256), acc[2 * w + 1] + terms(3, w, 1, 256, 256), 0)

    def near_terms(k, i, low, size):
        lhs = e_ring[:, quarter[k], :, :, low:low + size].reshape(4 * slots, size)
        return dot_t(lhs, w_buf[k, i // 2, i % 2, :, low:low + size])

    @scope("near")
    def near(k, low=0, size=512):
        for i in range(4):
            term = near_terms(k, i, low, size)
            acc_near[i] = term if k == 0 else acc_near[i] + term

    @scope("near_applied")
    def near_applied(w):
        real = acc_near[2 * w] + near_terms(3, 2 * w, 256, 256)
        imag = acc_near[2 * w + 1] + near_terms(3, 2 * w + 1, 256, 256)
        apply_to(w, z_down, real, imag, 0)
        apply_to(w, z_up, real, imag, 2 * slots)

    def x_pass(k):
        for way in range(2):
            x_copy(k, way, 1).wait_recv()
            x_copy(k, way, 2).start()

    def s_copy():
        ref = s_col.at[:, pl.ds(c * 8, 8)]
        return remote(ref, ref, s_send, s_recv, c=1 - c)

    with scope("ring0"):
        ring_pass(0)
    near(0)
    with scope("x_pass0"):
        x_pass(0)
    with scope("shared0"):
        shared(0)
    with scope("ring1"):
        ring_pass(1)
    near(1)
    near(2, 0, 256)
    with scope("shared1"):
        shared(1)
    near(3, 0, 256)
    with scope("wait_a"):
        to_a(0).wait_recv()
        to_a(1).wait_recv()
    for way in range(2):
        x_copy(1, way, 1).start()
    with scope("ring2"):
        ring_pass(2)
    near(2, 256, 256)
    with scope("wait_c"):
        pass_c(1).wait_recv()
    applied()
    with scope("shared2"):
        shared(2)
    near_applied(0)
    z_copy(0, 2, 0).start()
    near_applied(1)
    z_copy(1, 2, 1).start()
    z_copy(0, 2, 1).start()
    z_copy(1, 2, 0).start()
    look_up_some(5, 8)
    s_copy().start()
    with scope("x_pass1"):
        x_pass(1)
    with scope("turn"):
        s_copy().wait_recv()
        lax.fori_loop(0, 16, turn, 0)
    with scope("z20"):
        z_pass(2, 0)
    with scope("wait_x"):
        for k in range(2):
            for way in range(2):
                x_copy(k, way, 2).wait_recv()

    half = slots // 2
    deltas = (0, 7, 1, 6, 2, 5, 3, 4)

    def block_z(t):
        return lax.rem(z + deltas[t], 8)

    def mine(t):
        return lax.rem(block_z(t) // 2, 2) == c

    def across(t):
        return remote(x_send.at[t], x_recv.at[t], d_send, d_recv.at[t], c=1 - c)

    @scope("products")
    def products(t):
        zz = block_z(t)
        for w in range(2):
            y_swap[w, 0] = y_buf[w, zz, 1]
            y_swap[w, 1] = -y_buf[w, zz, 0]
        for i in range(2):
            real = e_plane[0, i * 4:i * 4 + 4].reshape(4 * slots, 512)
            imag = e_plane[1, i * 4:i * 4 + 4].reshape(4 * slots, 512)
            total = None
            for w in range(2):
                both = dot_t(real, y_buf[w, zz].reshape(2 * slots, 512)) + dot_t(imag, y_swap[w].reshape(2 * slots, 512))
                s = s_col[w, i * 4:i * 4 + 4].reshape(4 * slots, 128)
                factor = 0.5 * (jnp.concatenate([s, s[:, :2 * slots - 128]], axis=1) + s_row[w, zz][0:1])
                total = both * factor if total is None else total + both * factor
            total = total.reshape(4, slots, 2 * slots)
            s_sum[t % 2, i * 4:i * 4 + 4] = jnp.concatenate([total[:, :half], total[:, half:]], axis=2)

        @pl.when(jnp.logical_not(mine(t)))
        def _():
            x_send[t] = s_sum[t % 2].astype(BF16)
            across(t).start()

    def same_yl(t):
        return block_z(t) // 4 == yl

    def rows_of(t):
        return jnp.where(same_yl(t), yh, 1 - yh)

    def partner(t):
        return remote(h_send.at[t], h_recv.at[t], hs_send, hs_recv.at[t], yl=1 - yl)

    @scope("reduce")
    def reduce(t):
        @pl.when(mine(t))
        def _():
            across(t).wait_recv()
            here = rows_of(t) * 4
            there = 4 - here
            h_send[t] = (s_sum[t % 2, pl.ds(there, 4)] + x_recv[t, pl.ds(there, 4)].astype(F32)).astype(BF16)
            partner(t).start()
            h_keep[t] = s_sum[t % 2, pl.ds(here, 4)] + x_recv[t, pl.ds(here, 4)].astype(F32)

    def out_copy(t, dx):
        to_x = lax.rem(x + dx, 4)
        return remote(o_buf.at[t * 4 + to_x], o_recv.at[lax.rem(block_z(t), 2) * 16 + own_b], o_send, o_sem,
                      x=to_x, yh=rows_of(t), yl=jnp.where(same_yl(t), yl, 1 - yl))

    def keep(src, t):
        return pltpu.make_async_copy(src, o_recv.at[lax.rem(block_z(t), 2) * 16 + own_b], keep_sem)

    @scope("complete")
    def complete(t):
        @pl.when(mine(t))
        def _():
            partner(t).wait_recv()
            o_buf[t * 4:t * 4 + 4] = (h_keep[t] + h_recv[t].astype(F32)).astype(BF16)
            for dx in (2, 1, 3):
                out_copy(t, dx).start()

            @pl.when(same_yl(t))
            def _():
                keep(o_buf.at[t * 4 + x], t).start()

            @pl.when(jnp.logical_not(same_yl(t)))
            def _():
                out_copy(t, 0).start()

    last = len(deltas) - 1

    def last_copy(dyh, dx, same):
        to_yh, to_x = lax.rem(yh + dyh, 2), lax.rem(x + dx, 4)
        index = lax.rem(block_z(last), 2) * 16 + own_b + (0 if same else 8)
        return remote(last_buf.at[to_yh * 4 + to_x], o_recv.at[index], last_send, last_sem.at[0 if same else 1],
                      yh=to_yh, x=to_x, yl=yl if same else 1 - yl)

    @scope("finish")
    def finish():
        @pl.when(mine(last))
        def _():
            across(last).wait_recv()
            last_buf[...] = (s_sum[last % 2] + x_recv[last].astype(F32)).astype(BF16)
            for same in (True, False):
                @pl.when(same_yl(last) == same)
                def _():
                    for dx in (2, 1, 3, 0):
                        for dyh in (1, 0):
                            if dx or dyh or not same:
                                last_copy(dyh, dx, same).start()
                    if same:
                        keep(last_buf.at[own_b], last).start()

    products(0)
    products(1)
    with scope("z21"):
        z_pass(2, 1)
    reduce(0)
    products(2)
    reduce(1)
    products(3)
    reduce(2)
    products(4)
    reduce(3)
    complete(0)
    with scope("z30"):
        z_pass(3, 0)
    reduce(4)
    complete(1)
    complete(2)
    with scope("z31"):
        z_pass(3, 1)
    products(5)
    complete(3)
    products(6)
    reduce(5)
    complete(4)
    reduce(6)
    with scope("z40"):
        z_pass(4, 0)
    products(7)
    finish()
    complete(5)
    complete(6)

    def drain(ref, sem):
        remote(ref, ref, sem, sem, c=1 - c).wait_send()

    with scope("wait_out"):
        drain(e_full, p_send)
        drain(e_plane.at[:, 0:6], xr_send)
        drain(e_ring, er_send)
        s_copy().wait_send()
        drain(y_buf.at[:, 0:5], z_send)
        drain(x_send.at[0:4], d_send)
        keep(o_buf.at[0], 0).wait()
        keep(o_buf.at[0], 0).wait()

        @pl.when(jnp.logical_not(mine(last)))
        def _():
            drain(h_send.at[0:4], hs_send)
            drain(o_buf.at[0:14], o_send)

        @pl.when(mine(last))
        def _():
            drain(h_send.at[0:3], hs_send)
            for same in (True, False):
                @pl.when(same_yl(last) == same)
                def _():
                    drain(o_buf.at[0:11 if same else 10], o_send)
                    drain(last_buf.at[0:7 if same else 8], last_send)

        drain_in = lambda n, sem: remote(o_recv.at[0:n], o_recv.at[0:n], o_send, sem, c=1 - c).wait_recv()
        has_last = block_z(last) // 2 == own_q

        @pl.when(jnp.logical_not(has_last))
        def _():
            drain_in(14, o_sem)

        @pl.when(has_last)
        def _():
            drain_in(7, o_sem)
            drain_in(7, last_sem.at[0])
            drain_in(8, last_sem.at[1])


def lay_out(parts, out, held, laid, in_sem, out_sem):
    rows = laid.shape[2]
    half = rows // 2
    stores = []
    def split(i):
        mine = (lax.axis_index("yl") * 2 + lax.axis_index("c")) * 2 + i // 2
        return mine == lax.rem(lax.axis_index("z") + 4, 8)

    def load(i, side):
        at = i // 2 * 16 + side * 8 + i % 2 * 4
        return pltpu.make_async_copy(parts.at[pl.ds(at, 4)], held.at[i, side], in_sem.at[i, side])

    for i in range(4):
        load(i, 0).start()

        @pl.when(split(i))
        def _():
            load(i, 1).start()

        stores.append(pltpu.make_async_copy(laid.at[i], out.at[:, :, pl.ds(i * 4 * rows, 4 * rows)], out_sem.at[i]))

    def place(i, both):
        for b in range(4):
            block = held[i, 0, b].astype(F32)
            if both:
                block = block + held[i, 1, b].astype(F32)
            for part in range(2):
                for side in range(2):
                    at = (side * 2 + part) * rows
                    laid[i, part, side * half:side * half + half, b * rows:b * rows + rows] = block[:, at:at + rows]

    for i in range(4):
        load(i, 0).wait()

        @pl.when(split(i))
        def _():
            load(i, 1).wait()
            place(i, True)

        @pl.when(jnp.logical_not(split(i)))
        def _():
            place(i, False)

        stores[i].start()
    for store in stores:
            store.wait()


def on_device(elements, screened, energies, freq_points, freq_weights, band_of_slot):
    slots = elements.shape[1]
    half = slots // 2
    anywhere = pl.BlockSpec(memory_space=pl.ANY)
    dma = pltpu.SemaphoreType.DMA
    parts = pl.pallas_call(
        kernel,
        out_shape=jax.ShapeDtypeStruct((32, half, 4 * slots), BF16),
        in_specs=[anywhere] * 6,
        out_specs=anywhere,
        scratch_shapes=[
            pltpu.VMEM((4, 2, slots, 512), BF16),
            pltpu.VMEM((2, 4, 2, slots, 512), BF16),
            pltpu.VMEM((2, 8, slots, 512), BF16),
            pltpu.VMEM((4, 2, 2, 512, 512), BF16),
            pltpu.VMEM((4, 2 * slots, 512), F32),
            pltpu.VMEM((4, 4 * slots, 512), F32),
            pltpu.VMEM((2, 8, 2, slots, 512), BF16),
            pltpu.VMEM((2, 2, slots, 512), BF16),
            pltpu.VMEM((2, 8, half, 4 * slots), F32),
            pltpu.VMEM((8, 8, half, 4 * slots), BF16),
            pltpu.VMEM((8, 8, half, 4 * slots), BF16),
            pltpu.VMEM((8, 4, half, 4 * slots), BF16),
            pltpu.VMEM((8, 4, half, 4 * slots), BF16),
            pltpu.VMEM((8, 4, half, 4 * slots), F32),
            pltpu.VMEM((32, half, 4 * slots), BF16),
            pltpu.VMEM((8, half, 4 * slots), BF16),
            pltpu.VMEM((2, 16, slots, 128), F32),
            pltpu.VMEM((2, 8, 8, 2 * slots), F32),
            pltpu.VMEM((48, 128), F32),
            pltpu.VMEM((48, 128), jnp.int32),
            pltpu.VMEM((4, 16, 128), jnp.int32),
            pltpu.SMEM((2,), F32), pltpu.SMEM((2,), F32),
            dma((10,)), dma, dma((5,)), dma((2,)), dma, dma((2, 2, 2)),
            dma, dma((2, 3)), dma((2, 3)), dma, dma, dma, dma((2, 3, 2)),
            dma, dma((8,)), dma, dma((8,)), dma, dma, dma, dma, dma((2,)),
        ],
        compiler_params=pltpu.CompilerParams(
            collective_id=0, has_side_effects=True, vmem_limit_bytes=60 * 1024 * 1024),
        name="self_energy",
    )(elements, screened, energies.reshape(48, 128), band_of_slot.reshape(48, 128), freq_points, freq_weights)
    return pl.pallas_call(
        lay_out,
        out_shape=jax.ShapeDtypeStruct((2, slots, 16 * slots), F32),
        in_specs=[anywhere],
        out_specs=anywhere,
        scratch_shapes=[
            pltpu.VMEM((4, 2, 4, half, 4 * slots), BF16),
            pltpu.VMEM((4, 2, slots, 4 * slots), F32),
            dma((4, 2)), dma((4,)),
        ],
        compiler_params=pltpu.CompilerParams(vmem_limit_bytes=60 * 1024 * 1024),
        name="lay_out",
    )(parts)


def solution(mesh):
    torus = Mesh(mesh.devices.reshape(8, 2, 4, 2, 2), ("z", "yh", "x", "yl", "c"))
    return jax.shard_map(
        on_device,
        mesh=torus,
        in_specs=(P(None, BAND, GA), P(None, None, GA, None), P(), P(), P(), P()),
        out_specs=P(None, BAND, GA),
        check_vma=False,
    )
```

```python
import jax
import jax.numpy as jnp
from jax import lax
from jax.experimental import pallas as pl
from jax.experimental.pallas import tpu as pltpu
from jax.sharding import Mesh
from jax.sharding import PartitionSpec as P

BAND = ("z", "yh", "x")
GA = ("yl", "c")
F32 = jnp.float32
BF16 = jnp.bfloat16
scope = jax.named_scope


def dot_t(a, b):
    return lax.dot_general(a, b, (((1,), (1,)), ((), ())), preferred_element_type=F32)


def kernel(
    elements, screened, energies, bands, points, weights, o_recv,
    e_full, e_ring, e_plane, w_buf, acc, acc_near, y_buf, y_swap, s_sum, x_send, x_recv, h_send, h_recv, h_keep, o_buf, last_buf, s_col, s_row,
    energy_buf, band_buf, band_table, point_buf, weight_buf,
    load_sem, p_send, p_recv, a_recv, xr_send, xr_recv, er_send, er_recv, share_recv, s_send, s_recv, z_send, z_recv,
    d_send, d_recv, l_recv, hs_send, hs_recv, keep_sem, o_send, o_sem, last_send, last_sem,
):
    z, yh, x, yl, c = (lax.axis_index(name) for name in ("z", "yh", "x", "yl", "c"))
    own_q = yl * 2 + c
    own_b = yh * 4 + x
    slots = e_full.shape[2]

    def remote(src, dst, send, recv, **device):
        return pltpu.make_async_remote_copy(
            src_ref=src, dst_ref=dst, send_sem=send, recv_sem=recv,
            device_id=device, device_id_type=pl.DeviceIdType.MESH)

    quarter = [own_q, yl * 2 + (1 - c), (1 - yl) * 2 + c, (1 - yl) * 2 + (1 - c)]
    load_e = pltpu.make_async_copy(elements, e_full.at[own_q], load_sem.at[0])
    load_p = pltpu.make_async_copy(elements, e_plane.at[:, own_b], load_sem.at[1])
    load_e.start()
    load_p.start()
    load_s = [pltpu.make_async_copy(src, dst, load_sem.at[6 + i]) for i, (src, dst) in enumerate(
        ((energies, energy_buf), (bands, band_buf), (points, point_buf), (weights, weight_buf)))]
    load_w = []
    for k in range(4):
        at = pl.multiple_of(quarter[k] * 512, 512)
        load_w.append(pltpu.make_async_copy(screened.at[:, :, :, pl.ds(at, 512)], w_buf.at[k], load_sem.at[2 + k]))
        load_w[k].start()
    for load in load_s:
        load.start()

    barrier = pltpu.get_barrier_semaphore()

    def greet(**device):
        pl.semaphore_signal(barrier, inc=1, device_id=device, device_id_type=pl.DeviceIdType.MESH)

    def plane(dyh, dx, dyl):
        return dict(yh=lax.rem(yh + dyh, 2), x=lax.rem(x + dx, 4), yl=lax.rem(yl + dyl, 2))

    greet(c=1 - c)
    z_up, z_down = lax.rem(z + 1, 8), lax.rem(z + 7, 8)
    greet(z=z_up)
    greet(z=z_down)
    greet(yl=1 - yl)
    greet(yh=1 - yh, yl=1 - yl)
    greet(x=lax.rem(x + 1, 4))
    greet(x=lax.rem(x + 3, 4))
    with scope("enter"):
        pl.semaphore_wait(barrier, 7)
        load_e.wait()

    def to_y(h):
        ref = e_full.at[own_q, :, :, pl.ds(h * 256, 256)]
        return remote(ref, ref, p_send, p_recv.at[2 * h], yl=1 - yl)

    to_c = remote(e_full.at[own_q], e_full.at[own_q], p_send, p_recv.at[4], c=1 - c)
    to_y(0).start()
    to_y(1).start()
    to_c.start()
    load_p.wait()

    x_up, x_down = lax.rem(x + 1, 4), lax.rem(x + 3, 4)

    def block_at(k, at_x):
        return (yh if k == 0 else 1 - yh) * 4 + at_x

    def x_copy(k, way, hop):
        ahead, behind = (x_up, x_down) if way == 0 else (x_down, x_up)
        if hop == 1:
            ref = e_plane.at[:, block_at(k, x)]
        else:
            ref = e_plane.at[way, block_at(k, behind)]
        return remote(ref, ref, xr_send, xr_recv.at[k, way, hop - 1], x=ahead)

    def piece_of(ref, piece):
        if piece == 0:
            return ref.at[own_q]
        return ref.at[quarter[2], :, :, pl.ds((piece - 1) * 256, 256)]

    def ring(way, piece):
        return remote(piece_of(e_full, piece), piece_of(e_ring.at[way], piece), er_send, er_recv.at[way, piece],
                      z=z_up if way == 0 else z_down)

    def share(way, piece):
        ref = piece_of(e_ring.at[way], piece)
        return remote(ref, ref, er_send, share_recv.at[way, piece], c=1 - c)

    def ring_start(piece):
        for way in range(2):
            ring(way, piece).start()

    def ring_pass(piece):
        for way in range(2):
            ring(way, piece).wait_recv()
            share(way, piece).start()

    def shared(piece):
        for way in range(2):
            share(way, piece).wait_recv()

    ring_start(0)
    for way in range(2):
        x_copy(0, way, 1).start()

    def spread_bands():
        rows = [band_buf[pl.ds(k, 16, stride=3), :] for k in range(3)]
        band_table[0] = rows[0]
        band_table[1] = jnp.concatenate([rows[0][:, 96:], rows[1][:, :96]], axis=1)
        band_table[2] = jnp.concatenate([rows[1][:, 64:], rows[2][:, :64]], axis=1)
        band_table[3] = jnp.concatenate([rows[2][:, 32:], rows[2][:, :32]], axis=1)

    def look_up(i, carry):
        i = i + c * 8
        at = jnp.where(i < 8, z * 8 + i, (i - 8) * 8 + own_b)
        band = band_table[lax.rem(at, 4), pl.ds(at // 4, 1), :]
        band = jnp.broadcast_to(band, (128, 128)).T[:slots]
        lane = lax.broadcasted_iota(jnp.int32, (slots, 128), 1)

        def part(j, total):
            for u in range(8):
                row = j * 8 + u
                e = jnp.broadcast_to(energy_buf[pl.ds(row, 1), :], (slots, 128))
                total = total + jnp.where(band == lane + row * 128, e, 0.0)
            return total

        total = lax.fori_loop(0, 6, part, jnp.zeros((slots, 128), F32))
        energy = jnp.broadcast_to(jnp.sum(total, axis=1, keepdims=True), (slots, 128))
        for w in range(2):
            offset = energy - point_buf[w]
            s_col[w, i] = weight_buf[w] / (1.0 + 4.0 * offset * offset)
        return carry

    def turn(i, carry):
        w, g = i // 8, lax.rem(i, 8)
        one = s_col[w, 8 + g]
        s_row[w, g] = jnp.concatenate([one, one], axis=0).T[0:8]
        return carry

    def look_up_some(n, m):
        with scope("look_up"):
            lax.fori_loop(n, m, look_up, 0)

    def terms(k, w, part, low, size):
        lhs = e_full[quarter[k], :, :, low:low + size].reshape(2 * slots, size)
        return dot_t(lhs, w_buf[k, w, part, :, low:low + size])

    def accumulate(k, low=0, size=512):
        for i in range(4):
            term = terms(k, i // 2, i % 2, low, size)
            acc[i] = term if k == 0 else acc[i] + term

    with scope("quarter0"):
        load_w[0].wait()
        accumulate(0)

    with scope("quarter1"):
        to_c.wait_recv()
        load_w[1].wait()
        accumulate(1)

    def pass_c(h):
        ref = e_full.at[quarter[2], :, :, pl.ds(h * 256, 256)]
        return remote(ref, ref, p_send, p_recv.at[2 * h + 1], c=1 - c)

    other = e_full.at[quarter[2]]

    def to_a(h):
        cols = pl.ds(h * 256, 256)
        return remote(other.at[:, :, cols], e_plane.at[:, own_b, :, cols], p_send, a_recv.at[h], yh=1 - yh, yl=1 - yl)

    load_w[2].wait()
    load_w[3].wait()
    for load in load_s:
        load.wait()
    spread_bands()
    look_up_some(0, 3)
    with scope("wait_y0"):
        to_y(0).wait_recv()
    pass_c(0).start()
    ring_start(1)
    to_a(0).start()
    with scope("quarter2"):
        accumulate(2, 0, 256)
    look_up_some(3, 5)
    with scope("quarter2b"):
        pass_c(0).wait_recv()
        accumulate(3, 0, 256)
    with scope("wait_y1"):
        to_y(1).wait_recv()
    pass_c(1).start()
    ring_start(2)
    to_a(1).start()
    def z_copy(way, hop, w):
        ahead = z_up if way == 0 else z_down
        owner = lax.rem(z + 8 - (hop - 1), 8) if way == 0 else lax.rem(z + hop - 1, 8)
        ref = y_buf.at[w, owner]
        return remote(ref, ref, z_send, z_recv.at[way, hop - 2, w], z=ahead)

    def z_pass(hop, turn):
        for way in range(2):
            w = turn if way == 0 else 1 - turn
            z_copy(way, hop, w).wait_recv()
            if hop == 2 or (hop == 3 and turn == 0):
                z_copy(way, hop + 1, w).start()

    def apply_to(w, zz, real, imag, low):
        y_buf[w, zz, 0] = (real[low:low + slots] - imag[low + slots:low + 2 * slots]).astype(BF16)
        y_buf[w, zz, 1] = (imag[low:low + slots] + real[low + slots:low + 2 * slots]).astype(BF16)

    @scope("applied")
    def applied():
        for w in range(2):
            apply_to(w, z, acc[2 * w] + terms(3, w, 0, 256, 256), acc[2 * w + 1] + terms(3, w, 1, 256, 256), 0)

    def near_terms(k, i, low, size):
        lhs = e_ring[:, quarter[k], :, :, low:low + size].reshape(4 * slots, size)
        return dot_t(lhs, w_buf[k, i // 2, i % 2, :, low:low + size])

    @scope("near")
    def near(k, low=0, size=512):
        for i in range(4):
            term = near_terms(k, i, low, size)
            acc_near[i] = term if k == 0 else acc_near[i] + term

    @scope("near_applied")
    def near_applied(w):
        real = acc_near[2 * w] + near_terms(3, 2 * w, 256, 256)
        imag = acc_near[2 * w + 1] + near_terms(3, 2 * w + 1, 256, 256)
        apply_to(w, z_down, real, imag, 0)
        apply_to(w, z_up, real, imag, 2 * slots)

    def x_pass(k):
        for way in range(2):
            x_copy(k, way, 1).wait_recv()
            x_copy(k, way, 2).start()

    def s_copy():
        ref = s_col.at[:, pl.ds(c * 8, 8)]
        return remote(ref, ref, s_send, s_recv, c=1 - c)

    with scope("ring0"):
        ring_pass(0)
    near(0)
    with scope("x_pass0"):
        x_pass(0)
    with scope("quarter3"):
        accumulate(2, 256, 256)
    with scope("shared0"):
        shared(0)
    near(1)
    with scope("ring1"):
        ring_pass(1)
    near(2, 0, 256)
    with scope("wait_c"):
        pass_c(1).wait_recv()
    applied()
    with scope("shared1"):
        shared(1)
    near(3, 0, 256)
    with scope("wait_a"):
        to_a(0).wait_recv()
        to_a(1).wait_recv()
    for way in range(2):
        x_copy(1, way, 1).start()
    with scope("ring2"):
        ring_pass(2)
    near(2, 256, 256)
    with scope("shared2"):
        shared(2)
    near_applied(0)
    z_copy(0, 2, 0).start()
    near_applied(1)
    z_copy(1, 2, 1).start()
    z_copy(0, 2, 1).start()
    z_copy(1, 2, 0).start()
    look_up_some(5, 8)
    s_copy().start()
    with scope("x_pass1"):
        x_pass(1)
    with scope("turn"):
        s_copy().wait_recv()
        lax.fori_loop(0, 16, turn, 0)
    with scope("z20"):
        z_pass(2, 0)
    with scope("wait_x"):
        for k in range(2):
            for way in range(2):
                x_copy(k, way, 2).wait_recv()

    half = slots // 2
    deltas = (0, 7, 1, 6, 2, 5, 3, 4)

    def block_z(t):
        return lax.rem(z + deltas[t], 8)

    def mine(t):
        return lax.rem(block_z(t) // 2, 2) == c

    def across(t):
        return remote(x_send.at[t], x_recv.at[t], d_send, d_recv.at[t], c=1 - c)

    def swap(zz, ws=(0, 1)):
        for w in ws:
            y_swap[w, 0] = y_buf[w, zz, 1]
            y_swap[w, 1] = -y_buf[w, zz, 0]

    def rows_by_block(zz, at, ws=(0, 1)):
        real = e_plane[0, at].reshape(4 * slots, 512)
        imag = e_plane[1, at].reshape(4 * slots, 512)
        total = None
        for w in ws:
            both = dot_t(real, y_buf[w, zz].reshape(2 * slots, 512)) + dot_t(imag, y_swap[w].reshape(2 * slots, 512))
            s = s_col[w, at].reshape(4 * slots, 128)
            factor = 0.5 * (jnp.concatenate([s, s[:, :2 * slots - 128]], axis=1) + s_row[w, zz][0:1])
            total = both * factor if total is None else total + both * factor
        total = total.reshape(4, slots, 2 * slots)
        return jnp.concatenate([total[:, :half], total[:, half:]], axis=2)

    @scope("products_first")
    def products_first(t, w):
        zz = block_z(t)
        swap(zz, (w,))
        for i in range(2):
            at = pl.ds(i * 4, 4)
            s_sum[t % 2, at] = rows_by_block(zz, at, (w,))

    @scope("products")
    def products(t, w=None):
        zz = block_z(t)
        swap(zz, (0, 1) if w is None else (w,))
        for i in range(2):
            at = pl.ds(i * 4, 4)
            if w is None:
                s_sum[t % 2, at] = rows_by_block(zz, at)
            else:
                s_sum[t % 2, at] += rows_by_block(zz, at, (w,))

        @pl.when(jnp.logical_not(mine(t)))
        def _():
            x_send[t] = s_sum[t % 2].astype(BF16)
            across(t).start()

    def same_yl(t):
        return block_z(t) // 4 == yl

    def rows_of(t):
        return jnp.where(same_yl(t), yh, 1 - yh)

    def partner(t):
        return remote(h_send.at[t], h_recv.at[t], hs_send, hs_recv.at[t], yl=1 - yl)

    @scope("reduce")
    def reduce(t):
        @pl.when(mine(t))
        def _():
            across(t).wait_recv()
            here = rows_of(t) * 4
            there = 4 - here
            h_send[t] = (s_sum[t % 2, pl.ds(there, 4)] + x_recv[t, pl.ds(there, 4)].astype(F32)).astype(BF16)
            partner(t).start()
            h_keep[t] = s_sum[t % 2, pl.ds(here, 4)] + x_recv[t, pl.ds(here, 4)].astype(F32)

    def out_copy(t, dx):
        to_x = lax.rem(x + dx, 4)
        return remote(o_buf.at[t * 4 + to_x], o_recv.at[lax.rem(block_z(t), 2) * 16 + own_b], o_send, o_sem,
                      x=to_x, yh=rows_of(t), yl=jnp.where(same_yl(t), yl, 1 - yl))

    def keep(src, t):
        return pltpu.make_async_copy(src, o_recv.at[lax.rem(block_z(t), 2) * 16 + own_b], keep_sem)

    @scope("complete")
    def complete(t):
        @pl.when(mine(t))
        def _():
            partner(t).wait_recv()
            o_buf[t * 4:t * 4 + 4] = (h_keep[t] + h_recv[t].astype(F32)).astype(BF16)
            for dx in (2, 1, 3):
                out_copy(t, dx).start()

            @pl.when(same_yl(t))
            def _():
                keep(o_buf.at[t * 4 + x], t).start()

            @pl.when(jnp.logical_not(same_yl(t)))
            def _():
                out_copy(t, 0).start()

    last = len(deltas) - 1

    def last_copy(dyh, dx, same):
        to_yh, to_x = lax.rem(yh + dyh, 2), lax.rem(x + dx, 4)
        index = lax.rem(block_z(last), 2) * 16 + own_b + (0 if same else 8)
        return remote(last_buf.at[to_yh * 4 + to_x], o_recv.at[index], last_send, last_sem.at[0 if same else 1],
                      yh=to_yh, x=to_x, yl=yl if same else 1 - yl)

    def last_rows(p):
        return pl.ds((yh if p else 1 - yh) * 4, 4)

    def last_across(p):
        at = last_rows(p)
        return remote(x_send.at[last, at], x_recv.at[last, at], d_send, l_recv.at[p], c=1 - c)

    @scope("last_products")
    def last_products(p):
        zz, at = block_z(last), last_rows(p)
        if p == 0:
            swap(zz)
        s_sum[last % 2, at] = rows_by_block(zz, at)

        @pl.when(jnp.logical_not(mine(last)))
        def _():
            x_send[last, at] = s_sum[last % 2, at].astype(BF16)
            last_across(p).start()

    @scope("finish")
    def finish(p):
        at = last_rows(p)

        @pl.when(mine(last))
        def _():
            last_across(p).wait_recv()
            last_buf[at] = (s_sum[last % 2, at] + x_recv[last, at].astype(F32)).astype(BF16)
            for same in (True, False):
                @pl.when(same_yl(last) == same)
                def _():
                    for dx in (2, 1, 3, 0):
                        if dx or p == 0 or not same:
                            last_copy(1 - p, dx, same).start()
                    if same and p:
                        keep(last_buf.at[own_b], last).start()

    products(0)
    products(1)
    with scope("z21"):
        z_pass(2, 1)
    reduce(0)
    products(2)
    reduce(1)
    products(3)
    reduce(2)
    products(4)
    reduce(3)
    complete(0)
    with scope("z30"):
        z_pass(3, 0)
    reduce(4)
    products_first(5, 0)
    complete(1)
    products_first(6, 1)
    complete(2)
    with scope("z31"):
        z_pass(3, 1)
    products(5, 1)
    products(6, 0)
    reduce(5)
    complete(3)
    reduce(6)
    complete(4)
    with scope("z40"):
        z_pass(4, 0)
    last_products(0)
    last_products(1)
    finish(0)
    complete(5)
    finish(1)
    complete(6)

    def drain(ref, sem):
        remote(ref, ref, sem, sem, c=1 - c).wait_send()

    with scope("wait_out"):
        drain(e_full, p_send)
        drain(e_plane.at[:, 0:6], xr_send)
        drain(e_ring, er_send)
        s_copy().wait_send()
        drain(y_buf.at[:, 0:5], z_send)
        drain(x_send.at[0:4], d_send)
        keep(o_buf.at[0], 0).wait()
        keep(o_buf.at[0], 0).wait()

        @pl.when(jnp.logical_not(mine(last)))
        def _():
            drain(h_send.at[0:4], hs_send)
            drain(o_buf.at[0:14], o_send)

        @pl.when(mine(last))
        def _():
            drain(h_send.at[0:3], hs_send)
            for same in (True, False):
                @pl.when(same_yl(last) == same)
                def _():
                    drain(o_buf.at[0:11 if same else 10], o_send)
                    drain(last_buf.at[0:7 if same else 8], last_send)

        drain_in = lambda n, sem: remote(o_recv.at[0:n], o_recv.at[0:n], o_send, sem, c=1 - c).wait_recv()
        has_last = block_z(last) // 2 == own_q

        @pl.when(jnp.logical_not(has_last))
        def _():
            drain_in(14, o_sem)

        @pl.when(has_last)
        def _():
            drain_in(7, o_sem)
            drain_in(7, last_sem.at[0])
            drain_in(8, last_sem.at[1])


def lay_out(parts, out, held, laid, in_sem, out_sem):
    rows = laid.shape[2]
    half = rows // 2
    stores = []
    def split(i):
        mine = (lax.axis_index("yl") * 2 + lax.axis_index("c")) * 2 + i // 2
        return mine == lax.rem(lax.axis_index("z") + 4, 8)

    def load(i, side):
        at = i // 2 * 16 + side * 8 + i % 2 * 4
        return pltpu.make_async_copy(parts.at[pl.ds(at, 4)], held.at[i, side], in_sem.at[i, side])

    for i in range(4):
        load(i, 0).start()

        @pl.when(split(i))
        def _():
            load(i, 1).start()

        stores.append(pltpu.make_async_copy(laid.at[i], out.at[:, :, pl.ds(i * 4 * rows, 4 * rows)], out_sem.at[i]))

    def place(i, both):
        for b in range(4):
            block = held[i, 0, b].astype(F32)
            if both:
                block = block + held[i, 1, b].astype(F32)
            for part in range(2):
                for side in range(2):
                    at = (side * 2 + part) * rows
                    laid[i, part, side * half:side * half + half, b * rows:b * rows + rows] = block[:, at:at + rows]

    for i in range(4):
        load(i, 0).wait()

        @pl.when(split(i))
        def _():
            load(i, 1).wait()
            place(i, True)

        @pl.when(jnp.logical_not(split(i)))
        def _():
            place(i, False)

        stores[i].start()
    for store in stores:
            store.wait()


def on_device(elements, screened, energies, freq_points, freq_weights, band_of_slot):
    slots = elements.shape[1]
    half = slots // 2
    anywhere = pl.BlockSpec(memory_space=pl.ANY)
    dma = pltpu.SemaphoreType.DMA
    parts = pl.pallas_call(
        kernel,
        out_shape=jax.ShapeDtypeStruct((32, half, 4 * slots), BF16),
        in_specs=[anywhere] * 6,
        out_specs=anywhere,
        scratch_shapes=[
            pltpu.VMEM((4, 2, slots, 512), BF16),
            pltpu.VMEM((2, 4, 2, slots, 512), BF16),
            pltpu.VMEM((2, 8, slots, 512), BF16),
            pltpu.VMEM((4, 2, 2, 512, 512), BF16),
            pltpu.VMEM((4, 2 * slots, 512), F32),
            pltpu.VMEM((4, 4 * slots, 512), F32),
            pltpu.VMEM((2, 8, 2, slots, 512), BF16),
            pltpu.VMEM((2, 2, slots, 512), BF16),
            pltpu.VMEM((2, 8, half, 4 * slots), F32),
            pltpu.VMEM((8, 8, half, 4 * slots), BF16),
            pltpu.VMEM((8, 8, half, 4 * slots), BF16),
            pltpu.VMEM((8, 4, half, 4 * slots), BF16),
            pltpu.VMEM((8, 4, half, 4 * slots), BF16),
            pltpu.VMEM((8, 4, half, 4 * slots), F32),
            pltpu.VMEM((32, half, 4 * slots), BF16),
            pltpu.VMEM((8, half, 4 * slots), BF16),
            pltpu.VMEM((2, 16, slots, 128), F32),
            pltpu.VMEM((2, 8, 8, 2 * slots), F32),
            pltpu.VMEM((48, 128), F32),
            pltpu.VMEM((48, 128), jnp.int32),
            pltpu.VMEM((4, 16, 128), jnp.int32),
            pltpu.SMEM((2,), F32), pltpu.SMEM((2,), F32),
            dma((10,)), dma, dma((5,)), dma((2,)), dma, dma((2, 2, 2)),
            dma, dma((2, 3)), dma((2, 3)), dma, dma, dma, dma((2, 3, 2)),
            dma, dma((7,)), dma((2,)), dma, dma((7,)), dma, dma, dma, dma, dma((2,)),
        ],
        compiler_params=pltpu.CompilerParams(
            collective_id=0, has_side_effects=True, vmem_limit_bytes=60 * 1024 * 1024),
        name="self_energy",
    )(elements, screened, energies.reshape(48, 128), band_of_slot.reshape(48, 128), freq_points, freq_weights)
    return pl.pallas_call(
        lay_out,
        out_shape=jax.ShapeDtypeStruct((2, slots, 16 * slots), F32),
        in_specs=[anywhere],
        out_specs=anywhere,
        scratch_shapes=[
            pltpu.VMEM((4, 2, 4, half, 4 * slots), BF16),
            pltpu.VMEM((4, 2, slots, 4 * slots), F32),
            dma((4, 2)), dma((4,)),
        ],
        compiler_params=pltpu.CompilerParams(vmem_limit_bytes=60 * 1024 * 1024),
        name="lay_out",
    )(parts)


def solution(mesh):
    torus = Mesh(mesh.devices.reshape(8, 2, 4, 2, 2), ("z", "yh", "x", "yl", "c"))
    return jax.shard_map(
        on_device,
        mesh=torus,
        in_specs=(P(None, BAND, GA), P(None, None, GA, None), P(), P(), P(), P()),
        out_specs=P(None, BAND, GA),
        check_vma=False,
    )
```

```python
import jax
import jax.numpy as jnp
from jax import lax
from jax.experimental import pallas as pl
from jax.experimental.pallas import tpu as pltpu
from jax.sharding import Mesh
from jax.sharding import PartitionSpec as P

BAND = ("z", "yh", "x")
GA = ("yl", "c")
F32 = jnp.float32
BF16 = jnp.bfloat16
scope = jax.named_scope


def dot_t(a, b):
    return lax.dot_general(a, b, (((1,), (1,)), ((), ())), preferred_element_type=F32)


def kernel(
    elements, screened, energies, bands, points, weights, o_recv,
    e_full, e_ring, e_plane, w_buf, acc, acc_near, y_buf, y_swap, s_sum, x_send, x_recv, h_send, h_recv, h_keep, o_buf, last_buf, s_col, s_row,
    energy_buf, band_buf, band_table, point_buf, weight_buf,
    load_sem, p_send, p_recv, a_recv, xr_send, xr_recv, er_send, er_recv, share_recv, s_send, s_recv, z_send, z_recv,
    d_send, d_recv, l_recv, hs_send, hs_recv, keep_sem, o_send, o_sem, last_send, last_sem,
):
    z, yh, x, yl, c = (lax.axis_index(name) for name in ("z", "yh", "x", "yl", "c"))
    own_q = yl * 2 + c
    own_b = yh * 4 + x
    slots = e_full.shape[2]

    def remote(src, dst, send, recv, **device):
        return pltpu.make_async_remote_copy(
            src_ref=src, dst_ref=dst, send_sem=send, recv_sem=recv,
            device_id=device, device_id_type=pl.DeviceIdType.MESH)

    quarter = [own_q, yl * 2 + (1 - c), (1 - yl) * 2 + c, (1 - yl) * 2 + (1 - c)]
    load_e = pltpu.make_async_copy(elements, e_full.at[own_q], load_sem.at[0])
    load_p = pltpu.make_async_copy(elements, e_plane.at[:, own_b], load_sem.at[1])
    load_e.start()
    load_p.start()
    load_s = [pltpu.make_async_copy(src, dst, load_sem.at[6 + i]) for i, (src, dst) in enumerate(
        ((energies, energy_buf), (bands, band_buf), (points, point_buf), (weights, weight_buf)))]
    load_w = []
    for k in range(4):
        at = pl.multiple_of(quarter[k] * 512, 512)
        load_w.append(pltpu.make_async_copy(screened.at[:, :, :, pl.ds(at, 512)], w_buf.at[k], load_sem.at[2 + k]))
        load_w[k].start()
    for load in load_s:
        load.start()

    barrier = pltpu.get_barrier_semaphore()

    def greet(**device):
        pl.semaphore_signal(barrier, inc=1, device_id=device, device_id_type=pl.DeviceIdType.MESH)

    def plane(dyh, dx, dyl):
        return dict(yh=lax.rem(yh + dyh, 2), x=lax.rem(x + dx, 4), yl=lax.rem(yl + dyl, 2))

    greet(c=1 - c)
    z_up, z_down = lax.rem(z + 1, 8), lax.rem(z + 7, 8)
    greet(z=z_up)
    greet(z=z_down)
    greet(yl=1 - yl)
    greet(yh=1 - yh, yl=1 - yl)
    greet(x=lax.rem(x + 1, 4))
    greet(x=lax.rem(x + 3, 4))
    with scope("enter"):
        pl.semaphore_wait(barrier, 7)
        load_e.wait()

    def to_y(h):
        ref = e_full.at[own_q, :, :, pl.ds(h * 256, 256)]
        return remote(ref, ref, p_send, p_recv.at[2 * h], yl=1 - yl)

    to_c = remote(e_full.at[own_q], e_full.at[own_q], p_send, p_recv.at[4], c=1 - c)
    to_y(0).start()
    to_y(1).start()
    to_c.start()
    load_p.wait()

    x_up, x_down = lax.rem(x + 1, 4), lax.rem(x + 3, 4)

    def block_at(k, at_x):
        return (yh if k == 0 else 1 - yh) * 4 + at_x

    def x_copy(k, way, hop):
        ahead, behind = (x_up, x_down) if way == 0 else (x_down, x_up)
        if hop == 1:
            ref = e_plane.at[:, block_at(k, x)]
        else:
            ref = e_plane.at[way, block_at(k, behind)]
        return remote(ref, ref, xr_send, xr_recv.at[k, way, hop - 1], x=ahead)

    def piece_of(ref, piece):
        if piece == 0:
            return ref.at[own_q]
        return ref.at[quarter[2], :, :, pl.ds((piece - 1) * 256, 256)]

    def ring(way, piece):
        return remote(piece_of(e_full, piece), piece_of(e_ring.at[way], piece), er_send, er_recv.at[way, piece],
                      z=z_up if way == 0 else z_down)

    def share(way, piece):
        ref = piece_of(e_ring.at[way], piece)
        return remote(ref, ref, er_send, share_recv.at[way, piece], c=1 - c)

    def ring_start(piece):
        for way in range(2):
            ring(way, piece).start()

    def ring_pass(piece):
        for way in range(2):
            ring(way, piece).wait_recv()
            share(way, piece).start()

    def shared(piece):
        for way in range(2):
            share(way, piece).wait_recv()

    ring_start(0)
    for way in range(2):
        x_copy(0, way, 1).start()

    def spread_bands():
        rows = [band_buf[pl.ds(k, 16, stride=3), :] for k in range(3)]
        band_table[0] = rows[0]
        band_table[1] = jnp.concatenate([rows[0][:, 96:], rows[1][:, :96]], axis=1)
        band_table[2] = jnp.concatenate([rows[1][:, 64:], rows[2][:, :64]], axis=1)
        band_table[3] = jnp.concatenate([rows[2][:, 32:], rows[2][:, :32]], axis=1)

    def look_up(i, carry):
        i = i + c * 8
        at = jnp.where(i < 8, z * 8 + i, (i - 8) * 8 + own_b)
        band = band_table[lax.rem(at, 4), pl.ds(at // 4, 1), :]
        band = jnp.broadcast_to(band, (128, 128)).T[:slots]
        lane = lax.broadcasted_iota(jnp.int32, (slots, 128), 1)

        def part(j, total):
            for u in range(8):
                row = j * 8 + u
                e = jnp.broadcast_to(energy_buf[pl.ds(row, 1), :], (slots, 128))
                total = total + jnp.where(band == lane + row * 128, e, 0.0)
            return total

        total = lax.fori_loop(0, 6, part, jnp.zeros((slots, 128), F32))
        energy = jnp.broadcast_to(jnp.sum(total, axis=1, keepdims=True), (slots, 128))
        for w in range(2):
            offset = energy - point_buf[w]
            s_col[w, i] = weight_buf[w] / (1.0 + 4.0 * offset * offset)
        return carry

    def turn(i, carry):
        w, g = i // 8, lax.rem(i, 8)
        one = s_col[w, 8 + g]
        s_row[w, g] = jnp.concatenate([one, one], axis=0).T[0:8]
        return carry

    def look_up_some(n, m):
        with scope("look_up"):
            lax.fori_loop(n, m, look_up, 0)

    def terms(k, w, part, low, size):
        lhs = e_full[quarter[k], :, :, low:low + size].reshape(2 * slots, size)
        return dot_t(lhs, w_buf[k, w, part, :, low:low + size])

    def accumulate(k, low=0, size=512):
        for i in range(4):
            term = terms(k, i // 2, i % 2, low, size)
            acc[i] = term if k == 0 else acc[i] + term

    with scope("quarter0"):
        load_w[0].wait()
        accumulate(0)

    with scope("quarter1"):
        to_c.wait_recv()
        load_w[1].wait()
        accumulate(1)

    def pass_c(h):
        ref = e_full.at[quarter[2], :, :, pl.ds(h * 256, 256)]
        return remote(ref, ref, p_send, p_recv.at[2 * h + 1], c=1 - c)

    other = e_full.at[quarter[2]]

    def to_a(h):
        cols = pl.ds(h * 256, 256)
        return remote(other.at[:, :, cols], e_plane.at[:, own_b, :, cols], p_send, a_recv.at[h], yh=1 - yh, yl=1 - yl)

    load_w[2].wait()
    load_w[3].wait()
    for load in load_s:
        load.wait()
    spread_bands()
    look_up_some(0, 3)
    with scope("wait_y0"):
        to_y(0).wait_recv()
    pass_c(0).start()
    ring_start(1)
    to_a(0).start()
    with scope("quarter2"):
        accumulate(2, 0, 256)
    look_up_some(3, 5)
    with scope("quarter2b"):
        pass_c(0).wait_recv()
        accumulate(3, 0, 256)
    with scope("wait_y1"):
        to_y(1).wait_recv()
    pass_c(1).start()
    ring_start(2)
    to_a(1).start()
    def z_copy(way, hop, w):
        ahead = z_up if way == 0 else z_down
        owner = lax.rem(z + 8 - (hop - 1), 8) if way == 0 else lax.rem(z + hop - 1, 8)
        ref = y_buf.at[w, owner]
        return remote(ref, ref, z_send, z_recv.at[way, hop - 2, w], z=ahead)

    def z_pass(hop, turn):
        for way in range(2):
            w = turn if way == 0 else 1 - turn
            z_copy(way, hop, w).wait_recv()
            if hop == 2 or (hop == 3 and turn == 0):
                z_copy(way, hop + 1, w).start()

    def apply_to(w, zz, real, imag, low):
        y_buf[w, zz, 0] = (real[low:low + slots] - imag[low + slots:low + 2 * slots]).astype(BF16)
        y_buf[w, zz, 1] = (imag[low:low + slots] + real[low + slots:low + 2 * slots]).astype(BF16)

    @scope("applied")
    def applied():
        for w in range(2):
            apply_to(w, z, acc[2 * w] + terms(3, w, 0, 256, 256), acc[2 * w + 1] + terms(3, w, 1, 256, 256), 0)

    def near_terms(k, i, low, size):
        lhs = e_ring[:, quarter[k], :, :, low:low + size].reshape(4 * slots, size)
        return dot_t(lhs, w_buf[k, i // 2, i % 2, :, low:low + size])

    @scope("near")
    def near(k, low=0, size=512):
        for i in range(4):
            term = near_terms(k, i, low, size)
            acc_near[i] = term if k == 0 else acc_near[i] + term

    @scope("near_applied")
    def near_applied(w):
        real = acc_near[2 * w] + near_terms(3, 2 * w, 256, 256)
        imag = acc_near[2 * w + 1] + near_terms(3, 2 * w + 1, 256, 256)
        apply_to(w, z_down, real, imag, 0)
        apply_to(w, z_up, real, imag, 2 * slots)

    def x_pass(k):
        for way in range(2):
            x_copy(k, way, 1).wait_recv()
            x_copy(k, way, 2).start()

    def s_copy():
        ref = s_col.at[:, pl.ds(c * 8, 8)]
        return remote(ref, ref, s_send, s_recv, c=1 - c)

    with scope("ring0"):
        ring_pass(0)
    near(0)
    with scope("x_pass0"):
        x_pass(0)
    with scope("quarter3"):
        accumulate(2, 256, 256)
    with scope("shared0"):
        shared(0)
    near(1)
    with scope("ring1"):
        ring_pass(1)
    near(2, 0, 256)
    with scope("wait_c"):
        pass_c(1).wait_recv()
    applied()
    with scope("shared1"):
        shared(1)
    near(3, 0, 256)
    with scope("wait_a"):
        to_a(0).wait_recv()
        to_a(1).wait_recv()
    for way in range(2):
        x_copy(1, way, 1).start()
    with scope("ring2"):
        ring_pass(2)
    near(2, 256, 256)
    with scope("shared2"):
        shared(2)
    near_applied(0)
    z_copy(0, 2, 0).start()
    near_applied(1)
    z_copy(1, 2, 1).start()
    z_copy(0, 2, 1).start()
    z_copy(1, 2, 0).start()
    look_up_some(5, 8)
    s_copy().start()
    with scope("x_pass1"):
        x_pass(1)
    with scope("turn"):
        s_copy().wait_recv()
        lax.fori_loop(0, 16, turn, 0)
    with scope("z20"):
        z_pass(2, 0)
    with scope("wait_x"):
        for k in range(2):
            for way in range(2):
                x_copy(k, way, 2).wait_recv()

    half = slots // 2
    deltas = (0, 7, 1, 6, 2, 5, 3, 4)

    def block_z(t):
        return lax.rem(z + deltas[t], 8)

    def mine(t):
        return lax.rem(block_z(t) // 2, 2) == c

    def across(t):
        return remote(x_send.at[t], x_recv.at[t], d_send, d_recv.at[t], c=1 - c)

    def swap(zz, ws=(0, 1)):
        for w in ws:
            y_swap[w, 0] = y_buf[w, zz, 1]
            y_swap[w, 1] = -y_buf[w, zz, 0]

    def rows_by_block(zz, at, ws=(0, 1)):
        real = e_plane[0, at].reshape(4 * slots, 512)
        imag = e_plane[1, at].reshape(4 * slots, 512)
        total = None
        for w in ws:
            both = dot_t(real, y_buf[w, zz].reshape(2 * slots, 512)) + dot_t(imag, y_swap[w].reshape(2 * slots, 512))
            s = s_col[w, at].reshape(4 * slots, 128)
            factor = 0.5 * (jnp.concatenate([s, s[:, :2 * slots - 128]], axis=1) + s_row[w, zz][0:1])
            total = both * factor if total is None else total + both * factor
        total = total.reshape(4, slots, 2 * slots)
        return jnp.concatenate([total[:, :half], total[:, half:]], axis=2)

    @scope("products_first")
    def products_first(t, w):
        zz = block_z(t)
        swap(zz, (w,))
        for i in range(2):
            at = pl.ds(i * 4, 4)
            s_sum[t % 2, at] = rows_by_block(zz, at, (w,))

    @scope("products")
    def products(t, w=None):
        zz = block_z(t)
        swap(zz, (0, 1) if w is None else (w,))
        for i in range(2):
            at = pl.ds(i * 4, 4)
            if w is None:
                s_sum[t % 2, at] = rows_by_block(zz, at)
            else:
                s_sum[t % 2, at] += rows_by_block(zz, at, (w,))

        @pl.when(jnp.logical_not(mine(t)))
        def _():
            x_send[t] = s_sum[t % 2].astype(BF16)
            across(t).start()

    def same_yl(t):
        return block_z(t) // 4 == yl

    def rows_of(t):
        return jnp.where(same_yl(t), yh, 1 - yh)

    def partner(t):
        return remote(h_send.at[t], h_recv.at[t], hs_send, hs_recv.at[t], yl=1 - yl)

    @scope("reduce")
    def reduce(t):
        @pl.when(mine(t))
        def _():
            across(t).wait_recv()
            here = rows_of(t) * 4
            there = 4 - here
            h_send[t] = (s_sum[t % 2, pl.ds(there, 4)] + x_recv[t, pl.ds(there, 4)].astype(F32)).astype(BF16)
            partner(t).start()
            h_keep[t] = s_sum[t % 2, pl.ds(here, 4)] + x_recv[t, pl.ds(here, 4)].astype(F32)

    def out_copy(t, dx):
        to_x = lax.rem(x + dx, 4)
        return remote(o_buf.at[t * 4 + to_x], o_recv.at[lax.rem(block_z(t), 2) * 16 + own_b], o_send, o_sem,
                      x=to_x, yh=rows_of(t), yl=jnp.where(same_yl(t), yl, 1 - yl))

    def keep(src, t):
        return pltpu.make_async_copy(src, o_recv.at[lax.rem(block_z(t), 2) * 16 + own_b], keep_sem)

    @scope("complete")
    def complete(t):
        @pl.when(mine(t))
        def _():
            partner(t).wait_recv()
            o_buf[t * 4:t * 4 + 4] = (h_keep[t] + h_recv[t].astype(F32)).astype(BF16)
            for dx in (2, 3, 1):
                out_copy(t, dx).start()

            @pl.when(same_yl(t))
            def _():
                keep(o_buf.at[t * 4 + x], t).start()

            @pl.when(jnp.logical_not(same_yl(t)))
            def _():
                out_copy(t, 0).start()

    last = len(deltas) - 1

    def last_copy(dyh, dx, same):
        to_yh, to_x = lax.rem(yh + dyh, 2), lax.rem(x + dx, 4)
        index = lax.rem(block_z(last), 2) * 16 + own_b + (0 if same else 8)
        return remote(last_buf.at[to_yh * 4 + to_x], o_recv.at[index], last_send, last_sem.at[0 if same else 1],
                      yh=to_yh, x=to_x, yl=yl if same else 1 - yl)

    def last_rows(p):
        return pl.ds((yh if p else 1 - yh) * 4, 4)

    def last_across(p):
        at = last_rows(p)
        return remote(x_send.at[last, at], x_recv.at[last, at], d_send, l_recv.at[p], c=1 - c)

    @scope("last_products")
    def last_products(p):
        zz, at = block_z(last), last_rows(p)
        if p == 0:
            swap(zz)
        s_sum[last % 2, at] = rows_by_block(zz, at)

        @pl.when(jnp.logical_not(mine(last)))
        def _():
            x_send[last, at] = s_sum[last % 2, at].astype(BF16)
            last_across(p).start()

    @scope("finish")
    def finish(p):
        at = last_rows(p)

        @pl.when(mine(last))
        def _():
            last_across(p).wait_recv()
            last_buf[at] = (s_sum[last % 2, at] + x_recv[last, at].astype(F32)).astype(BF16)
            for same in (True, False):
                @pl.when(same_yl(last) == same)
                def _():
                    for dx in (2, 3, 1, 0):
                        if dx or p == 0 or not same:
                            last_copy(1 - p, dx, same).start()
                    if same and p:
                        keep(last_buf.at[own_b], last).start()

    products(0)
    products(1)
    with scope("z21"):
        z_pass(2, 1)
    reduce(0)
    products(2)
    reduce(1)
    products(3)
    reduce(2)
    products(4)
    reduce(3)
    complete(0)
    with scope("z30"):
        z_pass(3, 0)
    reduce(4)
    products_first(5, 0)
    complete(1)
    products_first(6, 1)
    complete(2)
    with scope("z31"):
        z_pass(3, 1)
    products(5, 1)
    products(6, 0)
    reduce(5)
    complete(3)
    reduce(6)
    complete(4)
    with scope("z40"):
        z_pass(4, 0)
    last_products(0)
    last_products(1)
    finish(0)
    complete(5)
    finish(1)
    complete(6)

    def drain(ref, sem):
        remote(ref, ref, sem, sem, c=1 - c).wait_send()

    with scope("wait_out"):
        drain(e_full, p_send)
        drain(e_plane.at[:, 0:6], xr_send)
        drain(e_ring, er_send)
        s_copy().wait_send()
        drain(y_buf.at[:, 0:5], z_send)
        drain(x_send.at[0:4], d_send)
        keep(o_buf.at[0], 0).wait()
        keep(o_buf.at[0], 0).wait()

        @pl.when(jnp.logical_not(mine(last)))
        def _():
            drain(h_send.at[0:4], hs_send)
            drain(o_buf.at[0:14], o_send)

        @pl.when(mine(last))
        def _():
            drain(h_send.at[0:3], hs_send)
            for same in (True, False):
                @pl.when(same_yl(last) == same)
                def _():
                    drain(o_buf.at[0:11 if same else 10], o_send)
                    drain(last_buf.at[0:7 if same else 8], last_send)

        drain_in = lambda n, sem: remote(o_recv.at[0:n], o_recv.at[0:n], o_send, sem, c=1 - c).wait_recv()
        has_last = block_z(last) // 2 == own_q

        @pl.when(jnp.logical_not(has_last))
        def _():
            drain_in(14, o_sem)

        @pl.when(has_last)
        def _():
            drain_in(7, o_sem)
            drain_in(7, last_sem.at[0])
            drain_in(8, last_sem.at[1])


def lay_out(parts, out, held, laid, in_sem, out_sem):
    rows = laid.shape[2]
    half = rows // 2
    stores = []
    def split(i):
        mine = (lax.axis_index("yl") * 2 + lax.axis_index("c")) * 2 + i // 2
        return mine == lax.rem(lax.axis_index("z") + 4, 8)

    def load(i, side):
        at = i // 2 * 16 + side * 8 + i % 2 * 4
        return pltpu.make_async_copy(parts.at[pl.ds(at, 4)], held.at[i, side], in_sem.at[i, side])

    for i in range(4):
        load(i, 0).start()

        @pl.when(split(i))
        def _():
            load(i, 1).start()

        stores.append(pltpu.make_async_copy(laid.at[i], out.at[:, :, pl.ds(i * 4 * rows, 4 * rows)], out_sem.at[i]))

    def place(i, both):
        for b in range(4):
            block = held[i, 0, b].astype(F32)
            if both:
                block = block + held[i, 1, b].astype(F32)
            for part in range(2):
                for side in range(2):
                    at = (side * 2 + part) * rows
                    laid[i, part, side * half:side * half + half, b * rows:b * rows + rows] = block[:, at:at + rows]

    for i in range(4):
        load(i, 0).wait()

        @pl.when(split(i))
        def _():
            load(i, 1).wait()
            place(i, True)

        @pl.when(jnp.logical_not(split(i)))
        def _():
            place(i, False)

        stores[i].start()
    for store in stores:
            store.wait()


def on_device(elements, screened, energies, freq_points, freq_weights, band_of_slot):
    slots = elements.shape[1]
    half = slots // 2
    anywhere = pl.BlockSpec(memory_space=pl.ANY)
    dma = pltpu.SemaphoreType.DMA
    parts = pl.pallas_call(
        kernel,
        out_shape=jax.ShapeDtypeStruct((32, half, 4 * slots), BF16),
        in_specs=[anywhere] * 6,
        out_specs=anywhere,
        scratch_shapes=[
            pltpu.VMEM((4, 2, slots, 512), BF16),
            pltpu.VMEM((2, 4, 2, slots, 512), BF16),
            pltpu.VMEM((2, 8, slots, 512), BF16),
            pltpu.VMEM((4, 2, 2, 512, 512), BF16),
            pltpu.VMEM((4, 2 * slots, 512), F32),
            pltpu.VMEM((4, 4 * slots, 512), F32),
            pltpu.VMEM((2, 8, 2, slots, 512), BF16),
            pltpu.VMEM((2, 2, slots, 512), BF16),
            pltpu.VMEM((2, 8, half, 4 * slots), F32),
            pltpu.VMEM((8, 8, half, 4 * slots), BF16),
            pltpu.VMEM((8, 8, half, 4 * slots), BF16),
            pltpu.VMEM((8, 4, half, 4 * slots), BF16),
            pltpu.VMEM((8, 4, half, 4 * slots), BF16),
            pltpu.VMEM((8, 4, half, 4 * slots), F32),
            pltpu.VMEM((32, half, 4 * slots), BF16),
            pltpu.VMEM((8, half, 4 * slots), BF16),
            pltpu.VMEM((2, 16, slots, 128), F32),
            pltpu.VMEM((2, 8, 8, 2 * slots), F32),
            pltpu.VMEM((48, 128), F32),
            pltpu.VMEM((48, 128), jnp.int32),
            pltpu.VMEM((4, 16, 128), jnp.int32),
            pltpu.SMEM((2,), F32), pltpu.SMEM((2,), F32),
            dma((10,)), dma, dma((5,)), dma((2,)), dma, dma((2, 2, 2)),
            dma, dma((2, 3)), dma((2, 3)), dma, dma, dma, dma((2, 3, 2)),
            dma, dma((7,)), dma((2,)), dma, dma((7,)), dma, dma, dma, dma, dma((2,)),
        ],
        compiler_params=pltpu.CompilerParams(
            collective_id=0, has_side_effects=True, vmem_limit_bytes=60 * 1024 * 1024),
        name="self_energy",
    )(elements, screened, energies.reshape(48, 128), band_of_slot.reshape(48, 128), freq_points, freq_weights)
    return pl.pallas_call(
        lay_out,
        out_shape=jax.ShapeDtypeStruct((2, slots, 16 * slots), F32),
        in_specs=[anywhere],
        out_specs=anywhere,
        scratch_shapes=[
            pltpu.VMEM((4, 2, 4, half, 4 * slots), BF16),
            pltpu.VMEM((4, 2, slots, 4 * slots), F32),
            dma((4, 2)), dma((4,)),
        ],
        compiler_params=pltpu.CompilerParams(vmem_limit_bytes=60 * 1024 * 1024),
        name="lay_out",
    )(parts)


def solution(mesh):
    torus = Mesh(mesh.devices.reshape(8, 2, 4, 2, 2), ("z", "yh", "x", "yl", "c"))
    return jax.shard_map(
        on_device,
        mesh=torus,
        in_specs=(P(None, BAND, GA), P(None, None, GA, None), P(), P(), P(), P()),
        out_specs=P(None, BAND, GA),
        check_vma=False,
    )
```

```python
import jax
import jax.numpy as jnp
from jax import lax
from jax.experimental import pallas as pl
from jax.experimental.pallas import tpu as pltpu
from jax.sharding import Mesh
from jax.sharding import PartitionSpec as P

BAND = ("z", "yh", "x")
GA = ("yl", "c")
F32 = jnp.float32
BF16 = jnp.bfloat16
scope = jax.named_scope


def dot_t(a, b):
    return lax.dot_general(a, b, (((1,), (1,)), ((), ())), preferred_element_type=F32)


def kernel(
    elements, screened, energies, bands, points, weights, o_recv,
    e_full, e_ring, e_plane, w_buf, acc, acc_near, y_buf, y_swap, s_sum, x_send, x_recv, h_send, h_recv, h_keep, o_buf, last_buf, s_col, s_row,
    energy_buf, band_buf, band_table, point_buf, weight_buf,
    load_sem, p_send, p_recv, a_recv, xr_send, xr_recv, er_send, er_recv, share_recv, s_send, s_recv, z_send, z_recv,
    d_send, d_recv, l_recv, hs_send, hs_recv, keep_sem, o_send, o_sem, last_send, last_sem,
):
    z, yh, x, yl, c = (lax.axis_index(name) for name in ("z", "yh", "x", "yl", "c"))
    own_q = yl * 2 + c
    own_b = yh * 4 + x
    slots = e_full.shape[2]

    def remote(src, dst, send, recv, **device):
        return pltpu.make_async_remote_copy(
            src_ref=src, dst_ref=dst, send_sem=send, recv_sem=recv,
            device_id=device, device_id_type=pl.DeviceIdType.MESH)

    quarter = [own_q, yl * 2 + (1 - c), (1 - yl) * 2 + c, (1 - yl) * 2 + (1 - c)]
    load_e = pltpu.make_async_copy(elements, e_full.at[own_q], load_sem.at[0])
    load_p = pltpu.make_async_copy(elements, e_plane.at[:, own_b], load_sem.at[1])
    load_e.start()
    load_p.start()
    load_s = [pltpu.make_async_copy(src, dst, load_sem.at[6 + i]) for i, (src, dst) in enumerate(
        ((energies, energy_buf), (bands, band_buf), (points, point_buf), (weights, weight_buf)))]
    load_w = []
    for k in range(4):
        at = pl.multiple_of(quarter[k] * 512, 512)
        load_w.append(pltpu.make_async_copy(screened.at[:, :, :, pl.ds(at, 512)], w_buf.at[k], load_sem.at[2 + k]))
        load_w[k].start()
    for load in load_s:
        load.start()

    barrier = pltpu.get_barrier_semaphore()

    def greet(**device):
        pl.semaphore_signal(barrier, inc=1, device_id=device, device_id_type=pl.DeviceIdType.MESH)

    def plane(dyh, dx, dyl):
        return dict(yh=lax.rem(yh + dyh, 2), x=lax.rem(x + dx, 4), yl=lax.rem(yl + dyl, 2))

    greet(c=1 - c)
    z_up, z_down = lax.rem(z + 1, 8), lax.rem(z + 7, 8)
    greet(z=z_up)
    greet(z=z_down)
    greet(yl=1 - yl)
    greet(yh=1 - yh, yl=1 - yl)
    greet(x=lax.rem(x + 1, 4))
    greet(x=lax.rem(x + 3, 4))
    with scope("enter"):
        pl.semaphore_wait(barrier, 7)
        load_e.wait()

    def to_y(h):
        ref = e_full.at[own_q, :, :, pl.ds(h * 256, 256)]
        return remote(ref, ref, p_send, p_recv.at[2 * h], yl=1 - yl)

    to_c = remote(e_full.at[own_q], e_full.at[own_q], p_send, p_recv.at[4], c=1 - c)
    to_y(0).start()
    to_y(1).start()
    to_c.start()
    load_p.wait()

    x_up, x_down = lax.rem(x + 1, 4), lax.rem(x + 3, 4)

    def block_at(k, at_x):
        return (yh if k == 0 else 1 - yh) * 4 + at_x

    def x_copy(k, way, hop):
        ahead, behind = (x_up, x_down) if way == 0 else (x_down, x_up)
        cols = pl.ds(0, 512) if k == 0 else pl.ds((k - 1) * 256, 256)
        if hop == 1:
            ref = e_plane.at[:, block_at(k, x), :, cols]
        else:
            ref = e_plane.at[way, block_at(k, behind), :, cols]
        return remote(ref, ref, xr_send, xr_recv.at[k, way, hop - 1], x=ahead)

    def piece_of(ref, piece):
        if piece == 0:
            return ref.at[own_q]
        return ref.at[quarter[2], :, :, pl.ds((piece - 1) * 256, 256)]

    def ring(way, piece):
        return remote(piece_of(e_full, piece), piece_of(e_ring.at[way], piece), er_send, er_recv.at[way, piece],
                      z=z_up if way == 0 else z_down)

    def share(way, piece):
        ref = piece_of(e_ring.at[way], piece)
        return remote(ref, ref, er_send, share_recv.at[way, piece], c=1 - c)

    def ring_start(piece):
        for way in range(2):
            ring(way, piece).start()

    def ring_pass(piece):
        for way in range(2):
            ring(way, piece).wait_recv()
            share(way, piece).start()

    def shared(piece):
        for way in range(2):
            share(way, piece).wait_recv()

    ring_start(0)
    for way in range(2):
        x_copy(0, way, 1).start()

    def spread_bands():
        rows = [band_buf[pl.ds(k, 16, stride=3), :] for k in range(3)]
        band_table[0] = rows[0]
        band_table[1] = jnp.concatenate([rows[0][:, 96:], rows[1][:, :96]], axis=1)
        band_table[2] = jnp.concatenate([rows[1][:, 64:], rows[2][:, :64]], axis=1)
        band_table[3] = jnp.concatenate([rows[2][:, 32:], rows[2][:, :32]], axis=1)

    def look_up(i, carry):
        i = i + c * 8
        at = jnp.where(i < 8, z * 8 + i, (i - 8) * 8 + own_b)
        band = band_table[lax.rem(at, 4), pl.ds(at // 4, 1), :]
        band = jnp.broadcast_to(band, (128, 128)).T[:slots]
        lane = lax.broadcasted_iota(jnp.int32, (slots, 128), 1)

        def part(j, total):
            for u in range(8):
                row = j * 8 + u
                e = jnp.broadcast_to(energy_buf[pl.ds(row, 1), :], (slots, 128))
                total = total + jnp.where(band == lane + row * 128, e, 0.0)
            return total

        total = lax.fori_loop(0, 6, part, jnp.zeros((slots, 128), F32))
        energy = jnp.broadcast_to(jnp.sum(total, axis=1, keepdims=True), (slots, 128))
        for w in range(2):
            offset = energy - point_buf[w]
            s_col[w, i] = weight_buf[w] / (1.0 + 4.0 * offset * offset)
        return carry

    def turn(i, carry):
        w, g = i // 8, lax.rem(i, 8)
        one = s_col[w, 8 + g]
        s_row[w, g] = jnp.concatenate([one, one], axis=0).T[0:8]
        return carry

    def look_up_some(n, m):
        with scope("look_up"):
            lax.fori_loop(n, m, look_up, 0)

    def terms(k, w, part, low, size):
        lhs = e_full[quarter[k], :, :, low:low + size].reshape(2 * slots, size)
        return dot_t(lhs, w_buf[k, w, part, :, low:low + size])

    def accumulate(k, low=0, size=512):
        for i in range(4):
            term = terms(k, i // 2, i % 2, low, size)
            acc[i] = term if k == 0 else acc[i] + term

    with scope("quarter0"):
        load_w[0].wait()
        accumulate(0)

    with scope("quarter1"):
        to_c.wait_recv()
        load_w[1].wait()
        accumulate(1)

    def pass_c(h):
        ref = e_full.at[quarter[2], :, :, pl.ds(h * 256, 256)]
        return remote(ref, ref, p_send, p_recv.at[2 * h + 1], c=1 - c)

    other = e_full.at[quarter[2]]

    def to_a(h):
        cols = pl.ds(h * 256, 256)
        return remote(other.at[:, :, cols], e_plane.at[:, own_b, :, cols], p_send, a_recv.at[h], yh=1 - yh, yl=1 - yl)

    load_w[2].wait()
    load_w[3].wait()
    for load in load_s:
        load.wait()
    spread_bands()
    look_up_some(0, 3)
    with scope("wait_y0"):
        to_y(0).wait_recv()
    pass_c(0).start()
    ring_start(1)
    to_a(0).start()
    with scope("quarter2"):
        accumulate(2, 0, 256)
    look_up_some(3, 5)
    with scope("quarter2b"):
        pass_c(0).wait_recv()
        accumulate(3, 0, 256)
    with scope("wait_y1"):
        to_y(1).wait_recv()
    pass_c(1).start()
    ring_start(2)
    to_a(1).start()
    def z_copy(way, hop, w):
        ahead = z_up if way == 0 else z_down
        owner = lax.rem(z + 8 - (hop - 1), 8) if way == 0 else lax.rem(z + hop - 1, 8)
        ref = y_buf.at[w, owner]
        return remote(ref, ref, z_send, z_recv.at[way, hop - 2, w], z=ahead)

    def z_pass(hop, turn):
        for way in range(2):
            w = turn if way == 0 else 1 - turn
            z_copy(way, hop, w).wait_recv()
            if hop == 2 or (hop == 3 and turn == 0):
                z_copy(way, hop + 1, w).start()

    def apply_to(w, zz, real, imag, low):
        y_buf[w, zz, 0] = (real[low:low + slots] - imag[low + slots:low + 2 * slots]).astype(BF16)
        y_buf[w, zz, 1] = (imag[low:low + slots] + real[low + slots:low + 2 * slots]).astype(BF16)

    @scope("applied")
    def applied():
        for w in range(2):
            apply_to(w, z, acc[2 * w] + terms(3, w, 0, 256, 256), acc[2 * w + 1] + terms(3, w, 1, 256, 256), 0)

    def near_terms(k, i, low, size):
        lhs = e_ring[:, quarter[k], :, :, low:low + size].reshape(4 * slots, size)
        return dot_t(lhs, w_buf[k, i // 2, i % 2, :, low:low + size])

    @scope("near")
    def near(k, low=0, size=512):
        for i in range(4):
            term = near_terms(k, i, low, size)
            acc_near[i] = term if k == 0 else acc_near[i] + term

    @scope("near_applied")
    def near_applied(w):
        real = acc_near[2 * w] + near_terms(3, 2 * w, 256, 256)
        imag = acc_near[2 * w + 1] + near_terms(3, 2 * w + 1, 256, 256)
        apply_to(w, z_down, real, imag, 0)
        apply_to(w, z_up, real, imag, 2 * slots)

    def x_pass(k):
        for way in range(2):
            x_copy(k, way, 1).wait_recv()
            x_copy(k, way, 2).start()

    def s_copy():
        ref = s_col.at[:, pl.ds(c * 8, 8)]
        return remote(ref, ref, s_send, s_recv, c=1 - c)

    with scope("ring0"):
        ring_pass(0)
    near(0)
    with scope("x_pass0"):
        x_pass(0)
    with scope("quarter3"):
        accumulate(2, 256, 256)
    with scope("shared0"):
        shared(0)
    near(1)
    with scope("ring1"):
        ring_pass(1)
    near(2, 0, 256)
    with scope("wait_a0"):
        to_a(0).wait_recv()
    for way in range(2):
        x_copy(1, way, 1).start()
    with scope("wait_c"):
        pass_c(1).wait_recv()
    applied()
    with scope("shared1"):
        shared(1)
    near(3, 0, 256)
    with scope("wait_a"):
        to_a(1).wait_recv()
    for way in range(2):
        x_copy(2, way, 1).start()
    with scope("ring2"):
        ring_pass(2)
    near(2, 256, 256)
    with scope("shared2"):
        shared(2)
    near_applied(0)
    z_copy(0, 2, 0).start()
    near_applied(1)
    z_copy(1, 2, 1).start()
    z_copy(0, 2, 1).start()
    z_copy(1, 2, 0).start()
    look_up_some(5, 8)
    s_copy().start()
    with scope("x_pass1"):
        x_pass(1)
        x_pass(2)
    with scope("turn"):
        s_copy().wait_recv()
        lax.fori_loop(0, 16, turn, 0)
    with scope("z20"):
        z_pass(2, 0)
    with scope("wait_x"):
        for k in range(3):
            for way in range(2):
                x_copy(k, way, 2).wait_recv()

    half = slots // 2
    deltas = (0, 7, 1, 6, 2, 5, 3, 4)

    def block_z(t):
        return lax.rem(z + deltas[t], 8)

    def mine(t):
        return lax.rem(block_z(t) // 2, 2) == c

    def across(t):
        return remote(x_send.at[t], x_recv.at[t], d_send, d_recv.at[t], c=1 - c)

    def swap(zz, ws=(0, 1)):
        for w in ws:
            y_swap[w, 0] = y_buf[w, zz, 1]
            y_swap[w, 1] = -y_buf[w, zz, 0]

    def rows_by_block(zz, at, ws=(0, 1)):
        real = e_plane[0, at].reshape(4 * slots, 512)
        imag = e_plane[1, at].reshape(4 * slots, 512)
        total = None
        for w in ws:
            both = dot_t(real, y_buf[w, zz].reshape(2 * slots, 512)) + dot_t(imag, y_swap[w].reshape(2 * slots, 512))
            s = s_col[w, at].reshape(4 * slots, 128)
            factor = 0.5 * (jnp.concatenate([s, s[:, :2 * slots - 128]], axis=1) + s_row[w, zz][0:1])
            total = both * factor if total is None else total + both * factor
        total = total.reshape(4, slots, 2 * slots)
        return jnp.concatenate([total[:, :half], total[:, half:]], axis=2)

    @scope("products_first")
    def products_first(t, w):
        zz = block_z(t)
        swap(zz, (w,))
        for i in range(2):
            at = pl.ds(i * 4, 4)
            s_sum[t % 2, at] = rows_by_block(zz, at, (w,))

    @scope("products")
    def products(t, w=None):
        zz = block_z(t)
        swap(zz, (0, 1) if w is None else (w,))
        for i in range(2):
            at = pl.ds(i * 4, 4)
            if w is None:
                s_sum[t % 2, at] = rows_by_block(zz, at)
            else:
                s_sum[t % 2, at] += rows_by_block(zz, at, (w,))

        @pl.when(jnp.logical_not(mine(t)))
        def _():
            x_send[t] = s_sum[t % 2].astype(BF16)
            across(t).start()

    def same_yl(t):
        return block_z(t) // 4 == yl

    def rows_of(t):
        return jnp.where(same_yl(t), yh, 1 - yh)

    def partner(t):
        return remote(h_send.at[t], h_recv.at[t], hs_send, hs_recv.at[t], yl=1 - yl)

    @scope("reduce")
    def reduce(t):
        @pl.when(mine(t))
        def _():
            across(t).wait_recv()
            here = rows_of(t) * 4
            there = 4 - here
            h_send[t] = (s_sum[t % 2, pl.ds(there, 4)] + x_recv[t, pl.ds(there, 4)].astype(F32)).astype(BF16)
            partner(t).start()
            h_keep[t] = s_sum[t % 2, pl.ds(here, 4)] + x_recv[t, pl.ds(here, 4)].astype(F32)

    def out_copy(t, dx):
        to_x = lax.rem(x + dx, 4)
        return remote(o_buf.at[t * 4 + to_x], o_recv.at[lax.rem(block_z(t), 2) * 16 + own_b], o_send, o_sem,
                      x=to_x, yh=rows_of(t), yl=jnp.where(same_yl(t), yl, 1 - yl))

    def keep(src, t):
        return pltpu.make_async_copy(src, o_recv.at[lax.rem(block_z(t), 2) * 16 + own_b], keep_sem)

    @scope("complete")
    def complete(t):
        @pl.when(mine(t))
        def _():
            partner(t).wait_recv()
            o_buf[t * 4:t * 4 + 4] = (h_keep[t] + h_recv[t].astype(F32)).astype(BF16)
            for dx in (2, 3, 1):
                out_copy(t, dx).start()

            @pl.when(same_yl(t))
            def _():
                keep(o_buf.at[t * 4 + x], t).start()

            @pl.when(jnp.logical_not(same_yl(t)))
            def _():
                out_copy(t, 0).start()

    last = len(deltas) - 1

    def last_copy(dyh, dx, same):
        to_yh, to_x = lax.rem(yh + dyh, 2), lax.rem(x + dx, 4)
        index = lax.rem(block_z(last), 2) * 16 + own_b + (0 if same else 8)
        return remote(last_buf.at[to_yh * 4 + to_x], o_recv.at[index], last_send, last_sem.at[0 if same else 1],
                      yh=to_yh, x=to_x, yl=yl if same else 1 - yl)

    def last_rows(p):
        return pl.ds((yh if p else 1 - yh) * 4, 4)

    def last_across(p):
        at = last_rows(p)
        return remote(x_send.at[last, at], x_recv.at[last, at], d_send, l_recv.at[p], c=1 - c)

    @scope("last_products")
    def last_products(p):
        zz, at = block_z(last), last_rows(p)
        if p == 0:
            swap(zz)
        s_sum[last % 2, at] = rows_by_block(zz, at)

        @pl.when(jnp.logical_not(mine(last)))
        def _():
            x_send[last, at] = s_sum[last % 2, at].astype(BF16)
            last_across(p).start()

    @scope("finish")
    def finish(p):
        at = last_rows(p)

        @pl.when(mine(last))
        def _():
            last_across(p).wait_recv()
            last_buf[at] = (s_sum[last % 2, at] + x_recv[last, at].astype(F32)).astype(BF16)
            for same in (True, False):
                @pl.when(same_yl(last) == same)
                def _():
                    for dx in (2, 3, 1, 0):
                        if dx or p == 0 or not same:
                            last_copy(1 - p, dx, same).start()
                    if same and p:
                        keep(last_buf.at[own_b], last).start()

    products(0)
    products(1)
    with scope("z21"):
        z_pass(2, 1)
    reduce(0)
    products(2)
    reduce(1)
    products(3)
    reduce(2)
    products(4)
    reduce(3)
    complete(0)
    with scope("z30"):
        z_pass(3, 0)
    reduce(4)
    products_first(5, 0)
    complete(1)
    products_first(6, 1)
    complete(2)
    with scope("z31"):
        z_pass(3, 1)
    products(5, 1)
    products(6, 0)
    reduce(5)
    complete(3)
    reduce(6)
    complete(4)
    with scope("z40"):
        z_pass(4, 0)
    last_products(0)
    last_products(1)
    finish(0)
    complete(5)
    finish(1)
    complete(6)

    def drain(ref, sem):
        remote(ref, ref, sem, sem, c=1 - c).wait_send()

    with scope("wait_out"):
        drain(e_full, p_send)
        drain(e_plane.at[:, 0:6], xr_send)
        drain(e_ring, er_send)
        s_copy().wait_send()
        drain(y_buf.at[:, 0:5], z_send)
        drain(x_send.at[0:4], d_send)
        keep(o_buf.at[0], 0).wait()
        keep(o_buf.at[0], 0).wait()

        @pl.when(jnp.logical_not(mine(last)))
        def _():
            drain(h_send.at[0:4], hs_send)
            drain(o_buf.at[0:14], o_send)

        @pl.when(mine(last))
        def _():
            drain(h_send.at[0:3], hs_send)
            for same in (True, False):
                @pl.when(same_yl(last) == same)
                def _():
                    drain(o_buf.at[0:11 if same else 10], o_send)
                    drain(last_buf.at[0:7 if same else 8], last_send)

        drain_in = lambda n, sem: remote(o_recv.at[0:n], o_recv.at[0:n], o_send, sem, c=1 - c).wait_recv()
        has_last = block_z(last) // 2 == own_q

        @pl.when(jnp.logical_not(has_last))
        def _():
            drain_in(14, o_sem)

        @pl.when(has_last)
        def _():
            drain_in(7, o_sem)
            drain_in(7, last_sem.at[0])
            drain_in(8, last_sem.at[1])


def lay_out(parts, out, held, laid, in_sem, out_sem):
    rows = laid.shape[2]
    half = rows // 2
    stores = []
    def split(i):
        mine = (lax.axis_index("yl") * 2 + lax.axis_index("c")) * 2 + i // 2
        return mine == lax.rem(lax.axis_index("z") + 4, 8)

    def load(i, side):
        at = i // 2 * 16 + side * 8 + i % 2 * 4
        return pltpu.make_async_copy(parts.at[pl.ds(at, 4)], held.at[i, side], in_sem.at[i, side])

    for i in range(4):
        load(i, 0).start()

        @pl.when(split(i))
        def _():
            load(i, 1).start()

        stores.append(pltpu.make_async_copy(laid.at[i], out.at[:, :, pl.ds(i * 4 * rows, 4 * rows)], out_sem.at[i]))

    def place(i, both):
        for b in range(4):
            block = held[i, 0, b].astype(F32)
            if both:
                block = block + held[i, 1, b].astype(F32)
            for part in range(2):
                for side in range(2):
                    at = (side * 2 + part) * rows
                    laid[i, part, side * half:side * half + half, b * rows:b * rows + rows] = block[:, at:at + rows]

    for i in range(4):
        load(i, 0).wait()

        @pl.when(split(i))
        def _():
            load(i, 1).wait()
            place(i, True)

        @pl.when(jnp.logical_not(split(i)))
        def _():
            place(i, False)

        stores[i].start()
    for store in stores:
            store.wait()


def on_device(elements, screened, energies, freq_points, freq_weights, band_of_slot):
    slots = elements.shape[1]
    half = slots // 2
    anywhere = pl.BlockSpec(memory_space=pl.ANY)
    dma = pltpu.SemaphoreType.DMA
    parts = pl.pallas_call(
        kernel,
        out_shape=jax.ShapeDtypeStruct((32, half, 4 * slots), BF16),
        in_specs=[anywhere] * 6,
        out_specs=anywhere,
        scratch_shapes=[
            pltpu.VMEM((4, 2, slots, 512), BF16),
            pltpu.VMEM((2, 4, 2, slots, 512), BF16),
            pltpu.VMEM((2, 8, slots, 512), BF16),
            pltpu.VMEM((4, 2, 2, 512, 512), BF16),
            pltpu.VMEM((4, 2 * slots, 512), F32),
            pltpu.VMEM((4, 4 * slots, 512), F32),
            pltpu.VMEM((2, 8, 2, slots, 512), BF16),
            pltpu.VMEM((2, 2, slots, 512), BF16),
            pltpu.VMEM((2, 8, half, 4 * slots), F32),
            pltpu.VMEM((8, 8, half, 4 * slots), BF16),
            pltpu.VMEM((8, 8, half, 4 * slots), BF16),
            pltpu.VMEM((8, 4, half, 4 * slots), BF16),
            pltpu.VMEM((8, 4, half, 4 * slots), BF16),
            pltpu.VMEM((8, 4, half, 4 * slots), F32),
            pltpu.VMEM((32, half, 4 * slots), BF16),
            pltpu.VMEM((8, half, 4 * slots), BF16),
            pltpu.VMEM((2, 16, slots, 128), F32),
            pltpu.VMEM((2, 8, 8, 2 * slots), F32),
            pltpu.VMEM((48, 128), F32),
            pltpu.VMEM((48, 128), jnp.int32),
            pltpu.VMEM((4, 16, 128), jnp.int32),
            pltpu.SMEM((2,), F32), pltpu.SMEM((2,), F32),
            dma((10,)), dma, dma((5,)), dma((2,)), dma, dma((3, 2, 2)),
            dma, dma((2, 3)), dma((2, 3)), dma, dma, dma, dma((2, 3, 2)),
            dma, dma((7,)), dma((2,)), dma, dma((7,)), dma, dma, dma, dma, dma((2,)),
        ],
        compiler_params=pltpu.CompilerParams(
            collective_id=0, has_side_effects=True, vmem_limit_bytes=60 * 1024 * 1024),
        name="self_energy",
    )(elements, screened, energies.reshape(48, 128), band_of_slot.reshape(48, 128), freq_points, freq_weights)
    return pl.pallas_call(
        lay_out,
        out_shape=jax.ShapeDtypeStruct((2, slots, 16 * slots), F32),
        in_specs=[anywhere],
        out_specs=anywhere,
        scratch_shapes=[
            pltpu.VMEM((4, 2, 4, half, 4 * slots), BF16),
            pltpu.VMEM((4, 2, slots, 4 * slots), F32),
            dma((4, 2)), dma((4,)),
        ],
        compiler_params=pltpu.CompilerParams(vmem_limit_bytes=60 * 1024 * 1024),
        name="lay_out",
    )(parts)


def solution(mesh):
    torus = Mesh(mesh.devices.reshape(8, 2, 4, 2, 2), ("z", "yh", "x", "yl", "c"))
    return jax.shard_map(
        on_device,
        mesh=torus,
        in_specs=(P(None, BAND, GA), P(None, None, GA, None), P(), P(), P(), P()),
        out_specs=P(None, BAND, GA),
        check_vma=False,
    )
```
